32 devices in a mesh: groups: 2 (over y), seq: 4 (over z), section: 2 (over x), mp: 2 (over core).
Axes of the slice: x: 2, y: 2, z: 4, core: 2. Of those that a mesh axis runs over, the one named last changes fastest.
Arguments:
- light_queries: bfloat16 [2048, 8192], P(('groups', 'seq'), ('section', 'mp')), parts along dimension 0, may hold values from -6 to 6
- light_keys: bfloat16 [2048, 8192], P(('groups', 'seq'), ('section', 'mp')), parts along dimension 0, may hold values from -6 to 6
- light_values: bfloat16 [2048, 8192], P(('groups', 'seq'), ('section', 'mp')), parts along dimension 0, may hold values from -6 to 6
- decay_log: float32 [2048, 64], P(('groups', 'seq'), ('section', 'mp')), parts along dimension 0, may hold values from -1 to 0
- norm_gain: float32 [8192], P(('section', 'mp')), may hold values from 0.25 to 1.75
- soft_queries: bfloat16 [2048, 8192], P(('groups', 'seq'), ('section', 'mp')), parts along dimension 0, may hold values from -150 to 150
- soft_keys: bfloat16 [2048, 1024], P(('groups', 'seq'), ('section', 'mp')), parts along dimension 0, may hold values from -6 to 6
- soft_values: bfloat16 [2048, 1024], P(('groups', 'seq'), ('section', 'mp')), parts along dimension 0, may hold values from -6 to 6
- lengths: int32 [8], P('groups'), parts along dimension 0, may hold values from 1 to 256, 768 in all
Outputs:
- light_out: bfloat16 [2048, 8192], P(('groups', 'seq'), ('section', 'mp')), parts along dimension 0
- soft_out: bfloat16 [2048, 8192], P(('groups', 'seq'), ('section', 'mp')), parts along dimension 0
The draws below stay inside these ranges and needn't reach their ends.
There are 2 independent parts, one for each index of `groups`. The reference program is written for one: setup_inputs(seed, part) draws one part's arguments, and reference() takes and returns one part's arrays. A program takes and returns all parts, laid end to end along the dimension named above; an argument that names none is the same for every part. Nothing has to cross between parts.
Inputs may be any that keep to these rules, and one draw needn't show every extreme that they name: The live tokens of a block stand at its first slots; the lengths sum to 768.
All inputs are finite; a program needn't handle non-finite values.
Results may differ from the reference program's by a relative error of at most 0.007.
Values may be sent and summed in bfloat16 or wider, within the bound.
A program may use at most 64 MiB of HBM per device.

```python
import math
import jax
import jax.numpy as jnp
import numpy as np
from jax import lax

QUERY_HEAD_COUNT = 64
KV_HEADS = 8
HEAD_DIM = 128
TOK_DEV = 256
TOKEN_SLOTS = 1024
N_SEQ = 4


def draw_decay_log(key, part):
    random_subkeys = jax.random.split(jax.random.fold_in(key, 3), 8)
    slow_share = 0.5
    slow_heads = jax.random.uniform(random_subkeys[0], (QUERY_HEAD_COUNT,)) < slow_share
    slow_rate = jax.random.uniform(random_subkeys[1], (QUERY_HEAD_COUNT,), minval=0.05, maxval=0.2) * math.log(10.0) / TOKEN_SLOTS
    fast_rate = 1.0 / jax.random.uniform(random_subkeys[2], (QUERY_HEAD_COUNT,), minval=30.0, maxval=50.0)
    head_decay_rate = jnp.where(slow_heads, slow_rate, fast_rate)
    block_count = TOKEN_SLOTS // TOK_DEV
    block_multiplier = jnp.repeat(jax.random.uniform(random_subkeys[3], (block_count, QUERY_HEAD_COUNT), minval=0.6, maxval=1.4), TOK_DEV, axis=0)
    slot_multiplier = jax.random.uniform(random_subkeys[4], (TOKEN_SLOTS, QUERY_HEAD_COUNT), minval=0.5, maxval=1.5)
    first_position = jax.random.randint(random_subkeys[5], (QUERY_HEAD_COUNT,), 0, TOKEN_SLOTS)
    position_gap = jax.random.randint(random_subkeys[7], (QUERY_HEAD_COUNT,), 1, TOKEN_SLOTS)
    second_position = (first_position + position_gap) % TOKEN_SLOTS
    group_length = jax.random.uniform(random_subkeys[6], (2, QUERY_HEAD_COUNT), minval=math.log(0.5), maxval=math.log(0.8))
    token_slot_index = jnp.arange(TOKEN_SLOTS)[:, None]
    token_groups = jnp.where(token_slot_index == first_position[None, :], group_length[0][None, :], 0.0)
    token_groups = token_groups + jnp.where(token_slot_index == second_position[None, :], group_length[1][None, :], 0.0)
    return (-head_decay_rate[None, :] * block_multiplier * slot_multiplier + token_groups).astype(jnp.float32)


def soft_pair(key):
    first_key, second_key = jax.random.split(jax.random.fold_in(key, 17))
    queries = jnp.clip(jax.random.normal(first_key, (TOKEN_SLOTS, QUERY_HEAD_COUNT * HEAD_DIM), jnp.float32), -6.0, 6.0)
    keys_drawn = jnp.clip(jax.random.normal(second_key, (TOKEN_SLOTS, KV_HEADS * HEAD_DIM), jnp.float32), -6.0, 6.0)
    return (queries, keys_drawn)


def draw_soft_queries(key, part):
    return soft_pair(key)[0].astype(jnp.bfloat16)


def draw_soft_keys(key, part):
    return soft_pair(key)[1].astype(jnp.bfloat16)


def block_levels(own_key, extent, cuts, least, largest):
    level, own = 1.0, jax.random.fold_in(own_key, 6)
    for dim, blocks in cuts:
        heights = jnp.exp(jax.random.uniform(jax.random.fold_in(own, dim), (blocks,), jnp.float32, least / len(cuts), largest / len(cuts)))
        level = level * jnp.repeat(heights, extent[dim] // blocks).reshape([-1 if axis == dim else 1 for axis in range(len(extent))])
    return level


def profile(amount, total, reach, lean):
    loads = [(1 << 20) // math.isqrt(rank ** lean) + 1 for rank in range(2, amount + 1)]
    rest, given = total - reach - (amount - 1), [1] * (amount - 1)
    while rest > 0:
        movable = [i for i in range(amount - 1) if given[i] < reach]
        mass, remaining = sum([loads[i] for i in movable]), rest
        for i in movable:
            more = min(reach - given[i], max(1, remaining * loads[i] // mass), rest)
            given[i] = given[i] + more
            rest = rest - more
    return np.array([reach] + given)


def uneven(own_key, amount, total, bound, slope):
    if amount == 2:
        one = jax.random.randint(own_key, (), max(1, total - bound), min(bound, total - 1) + 1)
        return jnp.stack([one, total - one])
    tallies = jnp.asarray(profile(amount, total, bound, slope), jnp.int32)
    couples = (amount - 1) // 2
    source_of, receiver = tallies[1:1 + 2 * couples:2], tallies[2:2 + 2 * couples:2]
    slack = jnp.minimum(source_of - 1, bound - receiver)
    passed = jax.random.randint(jax.random.fold_in(own_key, 1), (couples,), 0, 1 << 20) % (slack + 1)
    tallies = tallies.at[1:1 + 2 * couples:2].set(source_of - passed).at[2:2 + 2 * couples:2].set(receiver + passed)
    return tallies[jax.random.permutation(jax.random.fold_in(own_key, 2), amount)]


def centred(key, shape, spread, limit, pieces=(), held_as=jnp.bfloat16):
    array = jax.random.normal(key, shape, jnp.float32) * spread
    if len(pieces) > 0:
        array = block_levels(key, shape, pieces, -0.22, 0.18) * array
    return jnp.clip(array, min=-limit, max=limit).astype(held_as)


def setup_inputs(seed: int = 0, part: int = 0) -> dict:
    streams_of = jax.random.split(jax.random.key(seed), 10)
    own_keys = jax.random.split(jax.random.fold_in(streams_of[9], part), 10)
    return {
        "light_queries": centred(own_keys[0], (TOKEN_SLOTS, QUERY_HEAD_COUNT * HEAD_DIM), 1.0, 6.0, ((0, 4), (1, 4))),
        "light_keys": centred(own_keys[1], (TOKEN_SLOTS, QUERY_HEAD_COUNT * HEAD_DIM), 1.0, 6.0, ((0, 4), (1, 4))),
        "light_values": centred(own_keys[2], (TOKEN_SLOTS, QUERY_HEAD_COUNT * HEAD_DIM), 1.0, 6.0, ((0, 4), (1, 4))),
        "decay_log": draw_decay_log(jax.random.fold_in(jax.random.fold_in(streams_of[9], part), 71), part),
        "norm_gain": jnp.clip(1.0 + 0.15 * jax.random.normal(streams_of[4], (QUERY_HEAD_COUNT * HEAD_DIM,), jnp.float32), 0.25, 1.75),
        "soft_queries": draw_soft_queries(jax.random.fold_in(jax.random.fold_in(streams_of[9], part), 71), part),
        "soft_keys": draw_soft_keys(jax.random.fold_in(jax.random.fold_in(streams_of[9], part), 71), part),
        "soft_values": centred(own_keys[7], (TOKEN_SLOTS, KV_HEADS * HEAD_DIM), 1.0, 6.0, ((0, 4), (1, 4))),
        "lengths": uneven(own_keys[8], N_SEQ, TOKEN_SLOTS * 3 // 4, TOK_DEV, 2).astype(jnp.int32),
    }


EPSILON = 1e-06

def rounded(values):
    return lax.optimization_barrier(values.astype(jnp.bfloat16)).astype(jnp.float32)

def light_reference(light_queries, light_keys, light_values, decay_log, norm_gain, lengths):
    block_shape = (N_SEQ, TOK_DEV, QUERY_HEAD_COUNT, HEAD_DIM)
    queries = light_queries.reshape(block_shape).astype(jnp.float32)
    keys_all = light_keys.reshape(block_shape).astype(jnp.float32)
    values_all = light_values.reshape(block_shape).astype(jnp.float32)
    decays = decay_log.reshape(N_SEQ, TOK_DEV, QUERY_HEAD_COUNT)
    score_scale = HEAD_DIM ** (-0.5)
    token_slot_index = jnp.arange(TOK_DEV, dtype=jnp.int32)
    causal = token_slot_index[:, None] >= token_slot_index[None, :]
    gain_heads = norm_gain.reshape(QUERY_HEAD_COUNT, HEAD_DIM)

    def advance(entering, inputs):
        query_block, key_block, value_block, decay_block, length = inputs
        live_rows = token_slot_index < length
        masked = jnp.where(live_rows[:, None], decay_block, 0.0)
        running = jnp.cumsum(masked, axis=0)
        ending = running[-1]
        scores = jnp.einsum('thd,shd->hts', query_block, key_block)
        log_gaps = running.T[:, :, None] - running.T[:, None, :]
        allowed = causal[None] & live_rows[None, None, :]
        weights = jnp.where(allowed, jnp.exp(jnp.where(causal[None], log_gaps, 0.0)), 0.0)
        intra_weight = rounded(scores * score_scale * weights)
        inside = jnp.einsum('hts,shd->thd', intra_weight, value_block)
        across = jnp.einsum('thd,hde->the', query_block * score_scale, entering, precision=lax.Precision.HIGHEST) * jnp.exp(running)[:, :, None]
        combined = inside + across
        normed = combined * lax.rsqrt(lax.optimization_barrier(jnp.mean(combined * combined, axis=-1, keepdims=True)) + EPSILON) * gain_heads
        output = jnp.where(live_rows[:, None, None], normed, 0.0)
        fading = jnp.exp(ending[None, :] - running) * live_rows[:, None]
        block_keys = rounded(key_block * fading[:, :, None])
        block_state = jnp.einsum('thd,the->hde', block_keys, value_block)
        leaving = jnp.exp(ending)[:, None, None] * entering + block_state
        return (leaving, output)
    initial = jnp.zeros((QUERY_HEAD_COUNT, HEAD_DIM, HEAD_DIM), jnp.float32)
    final_state, outputs = lax.scan(advance, initial, (queries, keys_all, values_all, decays, lengths))
    return outputs.astype(jnp.bfloat16).reshape(TOKEN_SLOTS, QUERY_HEAD_COUNT * HEAD_DIM)

def soft_reference(soft_queries, soft_keys, soft_values, live_all):
    group_size = QUERY_HEAD_COUNT // KV_HEADS
    score_scale = HEAD_DIM ** (-0.5)
    queries = soft_queries.reshape(N_SEQ, TOK_DEV, KV_HEADS, group_size, HEAD_DIM)
    keys_all = soft_keys.reshape(TOKEN_SLOTS, KV_HEADS, HEAD_DIM).transpose(1, 0, 2)
    values_all = soft_values.reshape(TOKEN_SLOTS, KV_HEADS, HEAD_DIM).transpose(1, 0, 2)
    positions = jnp.arange(TOKEN_SLOTS, dtype=jnp.int32)

    def per_block(block_index):
        query_block = lax.dynamic_index_in_dim(queries, block_index, 0, keepdims=False)
        query_pos = block_index * TOK_DEV + jnp.arange(TOK_DEV, dtype=jnp.int32)
        allowed = (positions[None, :] <= query_pos[:, None]) & live_all[None, :]

        def per_head(inputs):
            query_head, key_head, value_head = inputs
            scores = jnp.einsum('tgd,sd->gts', query_head.astype(jnp.float32), key_head.astype(jnp.float32)) * score_scale
            scores = jnp.where(allowed[None], scores, -jnp.inf)
            row_peak = lax.optimization_barrier(jnp.max(scores, axis=-1, keepdims=True))
            probs_full = jnp.exp(scores - row_peak)
            row_total = lax.optimization_barrier(jnp.sum(probs_full, axis=-1))
            summed = jnp.einsum('gts,sd->tgd', rounded(probs_full), value_head.astype(jnp.float32))
            return summed / row_total.T[:, :, None]
        heads_out = lax.map(per_head, (query_block.transpose(1, 0, 2, 3), keys_all, values_all))
        return heads_out.transpose(1, 0, 2, 3).reshape(TOK_DEV, QUERY_HEAD_COUNT * HEAD_DIM)
    outputs = lax.map(per_block, jnp.arange(N_SEQ, dtype=jnp.int32))
    outputs = outputs.reshape(TOKEN_SLOTS, QUERY_HEAD_COUNT * HEAD_DIM)
    return jnp.where(live_all[:, None], outputs, 0.0).astype(jnp.bfloat16)

def reference(light_queries, light_keys, light_values, decay_log, norm_gain, soft_queries, soft_keys, soft_values, lengths):
    positions = jnp.arange(TOKEN_SLOTS, dtype=jnp.int32)
    live_all = positions % TOK_DEV < lengths[positions // TOK_DEV]
    light_out = light_reference(light_queries, light_keys, light_values, decay_log, norm_gain, lengths)
    soft_out = soft_reference(soft_queries, soft_keys, soft_values, live_all)
    return (light_out, soft_out)
```

```python
import functools
import math

import jax
import jax.numpy as jnp
from jax import lax
from jax.experimental import pallas as pl
from jax.experimental.pallas import tpu as pltpu
from jax.sharding import PartitionSpec as P

MESH = pl.DeviceIdType.MESH
LOG2E = 1.4426950408889634
LOW = -1e30
CHUNK = 2
UNIT = 4
FINISH = 4


def mm(a, b, dims=((1,), (0,)), precision=None):
    return lax.dot_general(
        a, b, (dims, ((), ())), precision=precision, preferred_element_type=jnp.float32
    )


def kernel(
    n, width,
    lq_hbm, lk_hbm, lv_hbm, decay_hbm, gain_hbm, sq_hbm, sk_hbm, sv_hbm, lengths,
    light_out, soft_out,
    lq, lk, lv, sq, decay, gain, kbuf, vbuf,
    padded, cols, rows, states, state_in, state_out, bias, acc, peak,
    local_sem, k_send, k_recv, v_send, v_recv, s_send, s_recv,
):
    me = lax.axis_index("seq")
    right = {"seq": me + 1}
    heads, toks = decay.shape
    kv_count = kbuf.shape[2] // width
    group = heads // kv_count
    chunks = heads // CHUNK
    scale = width ** (-0.5)
    bf16, f32 = jnp.bfloat16, jnp.float32

    copies = [
        pltpu.make_async_copy(src, dst, local_sem.at[i])
        for i, (src, dst) in enumerate((
            (sk_hbm, kbuf.at[0]), (sv_hbm, vbuf.at[0]), (decay_hbm, decay), (lk_hbm, lk),
            (lv_hbm, lv), (sq_hbm, sq), (lq_hbm, lq), (gain_hbm, gain),
        ))
    ]
    for copy in copies:
        copy.start()

    barrier = pltpu.get_barrier_semaphore()

    @pl.when(me > 0)
    def _():
        pl.semaphore_signal(barrier, inc=1, device_id={"seq": me - 1}, device_id_type=MESH)

    @pl.when(me < n - 1)
    def _():
        pl.semaphore_signal(barrier, inc=1, device_id=right, device_id_type=MESH)

    inner = (me > 0) & (me < n - 1)

    @pl.when(inner)
    def _():
        pl.semaphore_wait(barrier, 2)

    @pl.when(jnp.logical_not(inner))
    def _():
        pl.semaphore_wait(barrier, 1)

    def key_copy(step):
        return pltpu.make_async_remote_copy(
            src_ref=kbuf.at[step], dst_ref=kbuf.at[step + 1],
            send_sem=k_send.at[step], recv_sem=k_recv.at[step + 1],
            device_id=right, device_id_type=MESH,
        )

    def value_copy(step):
        return pltpu.make_async_remote_copy(
            src_ref=vbuf.at[step], dst_ref=vbuf.at[step + 1],
            send_sem=v_send.at[step], recv_sem=v_recv.at[step + 1],
            device_id=right, device_id_type=MESH,
        )

    def state_copy(c):
        piece = pl.ds(c * CHUNK, CHUNK)
        return pltpu.make_async_remote_copy(
            src_ref=state_out.at[piece], dst_ref=state_in.at[piece],
            send_sem=s_send.at[c], recv_sem=s_recv.at[c],
            device_id=right, device_id_type=MESH,
        )

    copies[0].wait()
    copies[1].wait()

    @pl.when(me < n - 1)
    def _():
        key_copy(0).start()
        value_copy(0).start()

    copies[2].wait()
    own = lengths[me]
    tok_col = lax.broadcasted_iota(jnp.int32, (toks, width), 0)
    live = tok_col < own
    padded[...] = jnp.zeros_like(padded)
    tok_lane = lax.broadcasted_iota(jnp.int32, (heads, toks), 1)
    masked = jnp.where(tok_lane < own, decay[...], 0.0)
    at0 = lax.broadcasted_iota(jnp.int32, (toks, toks), 0)
    at1 = lax.broadcasted_iota(jnp.int32, (toks, toks), 1)
    padded[:heads, :] = mm(masked, (at0 <= at1).astype(f32), precision=lax.Precision.HIGHEST)
    padded[:heads, :] = padded[:heads, :] * LOG2E
    rows[...] = padded[:heads, :]
    running = padded[...].T
    for h in range(heads):
        cols[h] = jnp.broadcast_to(running[:, h : h + 1], (toks, width))

    copies[3].wait()
    copies[4].wait()

    def head_lanes(h):
        return pl.ds(pl.multiple_of(h * width, width), width)

    def block_states(c, carry):
        hs = [c * CHUNK + j for j in range(CHUNK)]
        faded = []
        for h in hs:
            col = cols[h]
            fading = jnp.where(live, jnp.exp2(col[toks - 1 : toks, :] - col), 0.0)
            faded.append((lk[:, head_lanes(h)].astype(f32) * fading).astype(bf16).T)
        found = [mm(x, lv[:, head_lanes(h)]) for h, x in zip(hs, faded)]
        for h, state in zip(hs, found):
            states[h] = state
            state_out[h] = state.astype(bf16)

        @pl.when(me == 0)
        def _():
            state_copy(c).start()

        return carry

    lax.fori_loop(0, chunks, block_states, 0)

    copies[5].wait()
    factor = scale * LOG2E
    bias[...] = jnp.where(at0 <= at1, 0.0, LOW)
    part = min(UNIT, group)
    pad = acc.shape[1] - width
    lane_pos = lax.broadcasted_iota(jnp.int32, (pad, toks), 1)

    def arrive(step):
        key_copy(step - 1).wait_recv()
        value_copy(step - 1).wait_recv()

    def attend(step, first):
        if not first:
            @pl.when(me == n - 1)
            def _():
                arrive(step)

            known = lengths[me - step]
            key_live = tok_col < known

        units = [(g, i) for g in range(kv_count) for i in range(group // part)]
        for u, (g, i) in enumerate(units):
            if u == len(units) // 2:
                @pl.when((me < n - 1) & (step < me))
                def _():
                    arrive(step + 1)
                    key_copy(step + 1).start()
                    value_copy(step + 1).start()

            if i == 0:
                lanes_g = slice(g * width, (g + 1) * width)
                if first:
                    keys = kbuf[0, :, lanes_g]
                    values = vbuf[0, :, lanes_g].T
                    counted = jnp.ones((pad, toks), bf16)
                else:
                    keys = kbuf[step, :, lanes_g].astype(f32)
                    keys = jnp.where(key_live, keys, keys[0:1, :]).astype(bf16)
                    values = vbuf[step, :, lanes_g].astype(f32)
                    values = jnp.where(key_live, values, 0.0).astype(bf16).T
                    counted = jnp.where(lane_pos < known, 1.0, 0.0).astype(bf16)
                values = jnp.concatenate([values, counted], axis=0)
            hs = [g * group + i * part + j for j in range(part)]
            scores = [mm(keys, sq[:, h * width : (h + 1) * width], ((1,), (1,))) for h in hs]
            if first:
                scores = [x + bias[...] for x in scores]
                peaks = [jnp.max(x, axis=0, keepdims=True) for x in scores]
            else:
                olds = [peak[h] for h in hs]
                peaks = [
                    jnp.maximum(o, jnp.max(x, axis=0, keepdims=True)) for o, x in zip(olds, scores)
                ]
            probs = [jnp.exp2((x - p) * factor).astype(bf16) for x, p in zip(scores, peaks)]
            sums = [mm(values, x) for x in probs]
            if not first:
                sums = [
                    jnp.exp2((o - p) * factor) * acc[h] + x
                    for h, o, p, x in zip(hs, olds, peaks, sums)
                ]
            for h, p, x in zip(hs, peaks, sums):
                peak[h] = p
                acc[h] = x

    attend(0, True)

    def later(step, carry):
        attend(step, False)
        return carry

    lax.fori_loop(1, me + 1, later, 0)

    def finish_soft(c, carry):
        hs = [c * FINISH + j for j in range(FINISH)]
        results = [(acc[h, :width, :] / acc[h, width : width + 1, :]).T for h in hs]
        for h, x in zip(hs, results):
            soft_out[:, head_lanes(h)] = jnp.where(live, x, 0.0).astype(bf16)
        return carry

    lax.fori_loop(0, heads // FINISH, finish_soft, 0)

    copies[6].wait()
    copies[7].wait()

    @pl.when(me == 0)
    def _():
        state_in[...] = jnp.zeros_like(state_in)

    bias[...] = jnp.where(at0 >= at1, math.log2(scale), LOW)
    half = toks // 2

    def lightning(c, carry):
        hs = [c * CHUNK + j for j in range(CHUNK)]
        queries = [lq[:, head_lanes(h)] for h in hs]
        faded = [cols[h] for h in hs]
        insides = []
        for top in (True, False):
            size = half if top else toks
            span = slice(0, half) if top else slice(half, toks)
            raw = [
                mm(q[span, :], lk[:size, head_lanes(h)], ((1,), (1,))) for h, q in zip(hs, queries)
            ]
            weights = []
            for h, col, x in zip(hs, faded, raw):
                wide = jnp.concatenate([col[span, :]] * (size // width), axis=1)
                gaps = (wide - rows[pl.ds(h, 1), :][:, :size]) + bias[span, :size]
                weights.append((x * jnp.exp2(gaps)).astype(bf16))
            insides.append([mm(w, lv[:size, head_lanes(h)]) for h, w in zip(hs, weights)])
        insides = [jnp.concatenate(x, axis=0) for x in zip(*insides)]
        drops = [jnp.exp2(col) * scale for col in faded]

        @pl.when(me > 0)
        def _():
            state_copy(c).wait_recv()

            @pl.when(me < n - 1)
            def _():
                for h in hs:
                    kept = jnp.exp2(cols[h, toks - 1 : toks, :])
                    state_out[h] = (kept * state_in[h].astype(f32) + states[h]).astype(bf16)
                state_copy(c).start()

        across = [mm(q, state_in[h]) for h, q in zip(hs, queries)]
        combined = [i + a * d for i, a, d in zip(insides, across, drops)]
        means = [jnp.mean(x * x, axis=1, keepdims=True) for x in combined]
        for h, x, mean in zip(hs, combined, means):
            normed = x * lax.rsqrt(mean + 1e-06) * gain[pl.ds(h, 1), :]
            light_out[:, head_lanes(h)] = jnp.where(live, normed, 0.0).astype(bf16)
        return carry

    lax.fori_loop(0, chunks, lightning, 0)

    @pl.when(me < n - 1)
    def _():
        def sent_blocks(step, carry):
            key_copy(step).wait_send()
            value_copy(step).wait_send()
            return carry

        lax.fori_loop(0, me + 1, sent_blocks, 0)

        def sent_states(c, carry):
            state_copy(c).wait_send()
            return carry

        lax.fori_loop(0, chunks, sent_states, 0)


def body(n, lq, lk, lv, decay, gain, sq, sk, sv, lengths):
    toks, heads = decay.shape
    width = lq.shape[1] // heads
    kv = sk.shape[1]
    chunks = heads // CHUNK
    bf16, f32 = jnp.bfloat16, jnp.float32
    out = pltpu.VMEM(lq.shape, bf16)
    dma = pltpu.SemaphoreType.DMA
    anywhere = pl.BlockSpec(memory_space=pltpu.HBM)
    vmem = pl.BlockSpec(memory_space=pltpu.VMEM)
    light, soft = pl.pallas_call(
        functools.partial(kernel, n, width),
        out_shape=(out, out),
        in_specs=[anywhere] * 8 + [pl.BlockSpec(memory_space=pltpu.SMEM)],
        out_specs=(vmem, vmem),
        scratch_shapes=[
            pltpu.VMEM(lq.shape, bf16), pltpu.VMEM(lq.shape, bf16), pltpu.VMEM(lq.shape, bf16),
            pltpu.VMEM(sq.shape, bf16), pltpu.VMEM((heads, toks), f32),
            pltpu.VMEM((heads, width), f32),
            pltpu.VMEM((n, toks, kv), bf16), pltpu.VMEM((n, toks, kv), bf16),
            pltpu.VMEM((width, toks), f32), pltpu.VMEM((heads, toks, width), f32),
            pltpu.VMEM((heads, toks), f32),
            pltpu.VMEM((heads, width, width), f32),
            pltpu.VMEM((heads, width, width), bf16), pltpu.VMEM((heads, width, width), bf16),
            pltpu.VMEM((toks, toks), f32),
            pltpu.VMEM((heads, width + 16, toks), f32), pltpu.VMEM((heads, 1, toks), f32),
            dma((8,)), dma((n,)), dma((n,)), dma((n,)), dma((n,)), dma((chunks,)), dma((chunks,)),
        ],
        compiler_params=pltpu.CompilerParams(
            collective_id=0, has_side_effects=True, vmem_limit_bytes=58000000
        ),
        name="hybrid",
    )(lq, lk, lv, decay.T, gain.reshape(heads, width), sq, sk, sv, lengths)
    largest = jnp.finfo(bf16).max
    return tuple(jnp.minimum(x, largest) for x in (light, soft))


def solution(mesh):
    block = P(("groups", "seq"), ("section", "mp"))
    return jax.shard_map(
        functools.partial(body, mesh.shape["seq"]),
        mesh=mesh,
        in_specs=(block, block, block, block, P(("section", "mp")), block, block, block, P("groups")),
        out_specs=(block, block),
        check_vma=False,
    )
```

```python
import functools
import math

import jax
import jax.numpy as jnp
from jax import lax
from jax.experimental import pallas as pl
from jax.experimental.pallas import tpu as pltpu
from jax.sharding import PartitionSpec as P

MESH = pl.DeviceIdType.MESH
LOG2E = 1.4426950408889634
LOW = -1e30
CHUNK = 2
PIECES = 8
UNIT = 4
FINISH = 4


def mm(a, b, dims=((1,), (0,)), precision=None):
    return lax.dot_general(
        a, b, (dims, ((), ())), precision=precision, preferred_element_type=jnp.float32
    )


def can_pack(n, toks, width, heads, kv):
    return n == 4 and toks == 2 * width and heads >= 2 * kv // width


def kernel(
    n, width,
    lq_hbm, lk_hbm, lv_hbm, decay_hbm, gain_hbm, sq_hbm, sk_hbm, sv_hbm, lengths,
    light_out, soft_out,
    lq, lk, lv, sq, decay, gain, kvbuf,
    padded, cols, rows, states, state_in, state_out, bias, causal, insum, acc, peak, pack, spare, later_q,
    local_sem, kv_send, kv_recv, s_send, s_recv, q_send, q_recv,
):
    me = lax.axis_index("seq")
    right = {"seq": me + 1}
    heads, toks = decay.shape
    kv = kvbuf.shape[2] // 2
    kv_count = kv // width
    rows_piece = toks // PIECES
    half = toks // 2
    packed = can_pack(n, toks, width, heads, kv)
    tiles = 2 * kv // width
    last = n - 1
    group = heads // kv_count
    chunks = heads // CHUNK
    scale = width ** (-0.5)
    bf16, f32 = jnp.bfloat16, jnp.float32

    copies = [
        pltpu.make_async_copy(src, dst, local_sem.at[i])
        for i, (src, dst) in enumerate((
            (sk_hbm, kvbuf.at[0, :, :kv]), (sv_hbm, kvbuf.at[0, :, kv:]), (decay_hbm, decay), (lk_hbm, lk),
            (lv_hbm, lv), (sq_hbm, sq), (lq_hbm, lq), (gain_hbm, gain),
        ))
    ]
    for copy in copies:
        copy.start()

    barrier = pltpu.get_barrier_semaphore()

    @pl.when(me > 0)
    def _():
        pl.semaphore_signal(barrier, inc=1, device_id={"seq": me - 1}, device_id_type=MESH)

    @pl.when(me < n - 1)
    def _():
        pl.semaphore_signal(barrier, inc=1, device_id=right, device_id_type=MESH)

    inner = (me > 0) & (me < n - 1)

    @pl.when(inner)
    def _():
        pl.semaphore_wait(barrier, 2)

    @pl.when(jnp.logical_not(inner))
    def _():
        pl.semaphore_wait(barrier, 1)

    def kv_copy(step, p):
        piece = pl.ds(p * rows_piece, rows_piece)
        return pltpu.make_async_remote_copy(
            src_ref=kvbuf.at[step, piece], dst_ref=kvbuf.at[step + 1, piece],
            send_sem=kv_send.at[step, p], recv_sem=kv_recv.at[step + 1, p],
            device_id=right, device_id_type=MESH,
        )

    def state_copy(h):
        return pltpu.make_async_remote_copy(
            src_ref=state_out.at[h], dst_ref=state_in.at[h],
            send_sem=s_send.at[h], recv_sem=s_recv.at[h],
            device_id=right, device_id_type=MESH,
        )

    def pack_copy(k):
        step, p = divmod(k, PIECES)
        piece = pl.ds(p * rows_piece, rows_piece)
        return pltpu.make_async_remote_copy(
            src_ref=pack.at[pl.ds((k - PIECES // 2) * rows_piece, rows_piece)],
            dst_ref=kvbuf.at[step + 1, piece],
            send_sem=kv_send.at[step, p], recv_sem=kv_recv.at[step + 1, p],
            device_id=right, device_id_type=MESH,
        )

    query_copy = pltpu.make_async_remote_copy(
        src_ref=lq_hbm.at[:half], dst_ref=later_q, send_sem=q_send, recv_sem=q_recv,
        device_id={"seq": me - 1}, device_id_type=MESH,
    )
    packs = (me == n - 2) if packed else False
    unpacks = (me == last) if packed else False
    forwards = (me < n - 2) if packed else (me < last)

    if packed:
        @pl.when(unpacks)
        def _():
            query_copy.start()

    copies[0].wait()
    copies[1].wait()

    @pl.when(me < last)
    def _():
        for p in range(PIECES // 2):
            kv_copy(0, p).start()

    @pl.when(forwards)
    def _():
        for p in range(PIECES // 2, PIECES):
            kv_copy(0, p).start()

    copies[2].wait()
    own = lengths[me]
    if packed:
        ends = [lengths[b] for b in range(n)]
        short = ends[3] < half
        cut1 = jnp.where(short, ends[2] + ends[3] - toks, jnp.maximum(ends[2] - half, 0))
        cut0 = 2 * toks - ends[0]
    tok_col = lax.broadcasted_iota(jnp.int32, (toks, width), 0)
    live = tok_col < own
    padded[...] = jnp.zeros_like(padded)
    tok_lane = lax.broadcasted_iota(jnp.int32, (heads, toks), 1)
    masked = jnp.where(tok_lane < own, decay[...], 0.0)
    at0 = lax.broadcasted_iota(jnp.int32, (toks, toks), 0)
    at1 = lax.broadcasted_iota(jnp.int32, (toks, toks), 1)
    padded[:heads, :] = mm(masked, (at0 <= at1).astype(f32), precision=lax.Precision.HIGHEST)
    padded[:heads, :] = padded[:heads, :] * LOG2E
    rows[...] = padded[:heads, :]
    running = padded[...].T
    for h in range(heads):
        cols[h] = jnp.broadcast_to(running[:, h : h + 1], (toks, width))

    copies[3].wait()
    copies[4].wait()

    def head_lanes(h):
        return pl.ds(h * width if isinstance(h, int) else pl.multiple_of(h * width, width), width)

    def block_states(hs):
        faded = []
        for h in hs:
            col = cols[h]
            fading = jnp.where(live, jnp.exp2(col[toks - 1 : toks, :] - col), 0.0)
            faded.append((lk[:, head_lanes(h)].astype(f32) * fading).astype(bf16).T)
        found = [mm(x, lv[:, head_lanes(h)]) for h, x in zip(hs, faded)]
        for h, state in zip(hs, found):
            states[h] = state
            state_out[h] = state.astype(bf16)

    def insides(hs):
        parts = []
        for top in (True, False):
            size = half if top else toks
            span = slice(0, half) if top else slice(half, toks)
            raw = [mm(lq[span, head_lanes(h)], lk[:size, head_lanes(h)], ((1,), (1,))) for h in hs]
            weights = []
            for h, x in zip(hs, raw):
                wide = jnp.concatenate([cols[h, span, :]] * (size // width), axis=1)
                gaps = (wide - rows[h : h + 1, :size]) + causal[span, :size]
                weights.append((x * jnp.exp2(gaps)).astype(bf16))
            parts.append([mm(w, lv[:size, head_lanes(h)]) for h, w in zip(hs, weights)])
        for h, top, low in zip(hs, *parts):
            insum[h, :half, :] = top
            insum[h, half:, :] = low

    copies[5].wait()
    copies[6].wait()
    factor = scale * LOG2E
    bias[...] = jnp.where(at0 <= at1, 0.0, LOW)
    causal[...] = jnp.where(at0 >= at1, math.log2(scale), LOW)
    part = min(UNIT, group)
    units = heads // part
    pad = acc.shape[1] - width
    lane_pos = lax.broadcasted_iota(jnp.int32, (pad, toks), 1)

    def one_hot(size, span, shift, limit):
        dst = lax.broadcasted_iota(jnp.int32, (size, span), 0)
        src = lax.broadcasted_iota(jnp.int32, (size, span), 1)
        return jnp.where((src - dst == shift) & (src < limit), 1.0, 0.0).astype(bf16)

    def fill(j):
        start = j * rows_piece
        total = jnp.zeros((rows_piece, 2 * kv), f32)
        if start < half:
            at = lax.broadcasted_iota(jnp.int32, (rows_piece, 2 * kv), 0) + start
            tail = kvbuf[0, half + start : half + start + rows_piece, :].astype(f32)
            total = jnp.where(at < cut1, tail, total)
        low, high = max(0, start - half), min(toks, start + rows_piece)
        if low < high:
            hot = one_hot(rows_piece, high - low, start - low - cut1, ends[1] - low)
            total = total + mm(hot, kvbuf[1, low:high, :])
        if start >= toks:
            high = start - toks + rows_piece
            total = total + mm(one_hot(rows_piece, high, start - cut0, high), kvbuf[2, :high, :])
        pack[start : start + rows_piece, :] = total.astype(bf16)

    def arrive(step, u):
        each = PIECES // units
        for p in range(u * each, (u + 1) * each):
            needed = True if not packed else (me < last) | (step < last) | (p < PIECES // 2)

            @pl.when(needed)
            def _():
                kv_copy(step - 1, p).wait_recv()

            @pl.when(forwards)
            def _():
                kv_copy(step, p).start()

            if packed:
                for b in (1, 2) if not isinstance(step, int) else (step,):
                    @pl.when(packs & (step == b))
                    def _():
                        j = (b - 1) * PIECES + p
                        fill(j)
                        pack_copy(PIECES // 2 + j).start()

    def pass_states(hs):
        for h in hs:
            state_copy(h).wait_recv()
            kept = jnp.exp2(cols[h, toks - 1 : toks, :])
            state_out[h] = (kept * state_in[h].astype(f32) + states[h]).astype(bf16)
            if packed:
                @pl.when(packs)
                def _():
                    out = state_out[h]
                    found = mm(later_q[:, head_lanes(h)], out)
                    extra = spare[jnp.minimum(h, tiles - 1)]
                    out = jnp.where(state_row < spare_end, extra, out.astype(f32))
                    state_out[h] = jnp.where(state_row < result_end, found, out).astype(bf16)

            state_copy(h).start()

    def unpack():
        for h in range(tiles):
            state_copy(h).wait_recv()
        for h in range(tiles):
            kvbuf[last, half:, h * width : (h + 1) * width] = state_in[h]

    def ranges(step):
        if not packed:
            return lengths[me - step], toks, toks, toks
        flat = lengths[jnp.maximum(me - step, 0)]
        joint = cut1 + ends[1]
        at = [step == k for k in range(n)]

        def pick(plain, one, two, three):
            return jnp.where(unpacks, jnp.where(at[1], one, jnp.where(at[2], two, three)), plain)

        return (
            pick(flat, jnp.minimum(ends[2], half), joint - half, jnp.minimum(joint - toks - half, half)),
            pick(toks, half, toks, cut0 - toks - half),
            pick(toks, half + joint, toks, half),
            pick(toks, toks, cut0 - half, jnp.where(short, half + ends[3], toks)),
        )

    def within(at, limits):
        a, b, c, d = limits
        return (at < a) | ((at >= b) & (at < c)) | (at >= d)

    def attend(step, u, shared):
        first = isinstance(step, int)
        g, i = divmod(u, group // part)
        if i == 0:
            lanes_g = slice(g * width, (g + 1) * width)
            lanes_v = slice(kv + g * width, kv + (g + 1) * width)
            if first:
                keys = kvbuf[0, :, lanes_g]
                values = kvbuf[0, :, lanes_v].T
                counted = jnp.ones((pad, toks), bf16)
            else:
                limits = ranges(step)
                key_live = within(tok_col, limits)
                seen = kvbuf[0, 0:1, lanes_g].astype(f32)
                keys = kvbuf[step, :, lanes_g].astype(f32)
                keys = jnp.where(key_live, keys, seen).astype(bf16)
                values = kvbuf[step, :, lanes_v].astype(f32)
                values = jnp.where(key_live, values, 0.0).astype(bf16).T
                counted = jnp.where(within(lane_pos, limits), 1.0, 0.0).astype(bf16)
            shared[:] = [keys, jnp.concatenate([values, counted], axis=0)]
        keys, values = shared
        hs = [g * group + i * part + j for j in range(part)]
        scores = [mm(keys, sq[:, h * width : (h + 1) * width], ((1,), (1,))) for h in hs]
        if first:
            scores = [x + bias[...] for x in scores]
            peaks = [jnp.max(x, axis=0, keepdims=True) for x in scores]
        else:
            olds = [peak[h] for h in hs]
            peaks = [
                jnp.maximum(o, jnp.max(x, axis=0, keepdims=True)) for o, x in zip(olds, scores)
            ]
        probs = [jnp.exp2((x - p) * factor).astype(bf16) for x, p in zip(scores, peaks)]
        sums = [mm(values, x) for x in probs]
        if not first:
            sums = [
                jnp.exp2((o - p) * factor) * acc[h] + x
                for h, o, p, x in zip(hs, olds, peaks, sums)
            ]
        for h, p, x in zip(hs, peaks, sums):
            peak[h] = p
            acc[h] = x

    shared = []
    for u in range(units):
        @pl.when(me > 0)
        def _():
            arrive(1, u)

        attend(0, u, shared)
        hs = range(u * part, (u + 1) * part)
        block_states(hs)
        insides(hs)

        @pl.when(me == 0)
        def _():
            for h in hs:
                state_copy(h).start()

    if packed:
        state_row = lax.broadcasted_iota(jnp.int32, (width, width), 0)
        result_end = jnp.where(short, ends[3], 0)
        spare_end = jnp.where(short, width, 0)
        across_end = jnp.where(unpacks & short, half, 0)

    relays = (me > 0) & (me < last)
    early = heads // 2

    def later(step, carry):
        if packed:
            @pl.when(unpacks & (step == last))
            def _():
                unpack()

            @pl.when(packs & (step == me))
            def _():
                query_copy.wait_recv()
                moved = mm(one_hot(half, toks, ends[2] - half, toks), kvbuf[0])
                for h in range(tiles):
                    spare[h] = moved[:, h * width : (h + 1) * width]

        shared = []
        for u in range(units):
            @pl.when(step < me)
            def _():
                arrive(step + 1, u)

            @pl.when(relays & (step == me))
            def _():
                each = early // units
                pass_states(range(u * each, (u + 1) * each))

            attend(step, u, shared)
        return carry

    lax.fori_loop(1, me + 1, later, 0)

    def finish_soft(c, carry):
        hs = [c * FINISH + j for j in range(FINISH)]
        results = [(acc[h, :width, :] / acc[h, width : width + 1, :]).T for h in hs]
        for h, x in zip(hs, results):
            soft_out[:, head_lanes(h)] = jnp.where(live, x, 0.0).astype(bf16)
        return carry

    lax.fori_loop(0, heads // FINISH, finish_soft, 0)

    copies[7].wait()

    @pl.when(me == 0)
    def _():
        state_in[...] = jnp.zeros_like(state_in)

    def lightning(c, carry):
        hs = [c * CHUNK + j for j in range(CHUNK)]

        @pl.when(relays & (c < chunks // 2))
        def _():
            pass_states([h + early for h in hs])

        @pl.when((me == last) & (c >= tiles // CHUNK if packed else True))
        def _():
            for h in hs:
                state_copy(h).wait_recv()

        across = [mm(lq[:, head_lanes(h)], state_in[h]) for h in hs]
        if packed:
            results = [state_in[h].astype(f32) for h in hs]
            results = [jnp.concatenate([x] * (toks // width), axis=0) for x in results]
            across = [jnp.where(tok_col < across_end, x, y) for x, y in zip(results, across)]
        drops = [jnp.exp2(cols[h]) * scale for h in hs]
        combined = [insum[h] + a * d for h, a, d in zip(hs, across, drops)]
        means = [jnp.mean(x * x, axis=1, keepdims=True) for x in combined]
        for h, x, mean in zip(hs, combined, means):
            normed = x * lax.rsqrt(mean + 1e-06) * gain[pl.ds(h, 1), :]
            light_out[:, head_lanes(h)] = jnp.where(live, normed, 0.0).astype(bf16)
        return carry

    lax.fori_loop(0, chunks, lightning, 0)

    if packed:
        @pl.when(unpacks)
        def _():
            query_copy.wait_send()

    @pl.when(me < n - 1)
    def _():
        def sent_blocks(step, carry):
            for p in range(PIECES):
                sent = True if not packed else (me < n - 2) | (step < n - 2) | (p < PIECES // 2)

                @pl.when(sent)
                def _():
                    kv_copy(step, p).wait_send()

            return carry

        lax.fori_loop(0, me + 1, sent_blocks, 0)

        def sent_states(h, carry):
            state_copy(h).wait_send()
            return carry

        lax.fori_loop(0, heads, sent_states, 0)


def body(n, lq, lk, lv, decay, gain, sq, sk, sv, lengths):
    toks, heads = decay.shape
    width = lq.shape[1] // heads
    kv = sk.shape[1]
    chunks = heads // CHUNK
    bf16, f32 = jnp.bfloat16, jnp.float32
    out = pltpu.VMEM(lq.shape, bf16)
    dma = pltpu.SemaphoreType.DMA
    anywhere = pl.BlockSpec(memory_space=pltpu.HBM)
    vmem = pl.BlockSpec(memory_space=pltpu.VMEM)
    light, soft = pl.pallas_call(
        functools.partial(kernel, n, width),
        out_shape=(out, out),
        in_specs=[anywhere] * 8 + [pl.BlockSpec(memory_space=pltpu.SMEM)],
        out_specs=(vmem, vmem),
        scratch_shapes=[
            pltpu.VMEM(lq.shape, bf16), pltpu.VMEM(lq.shape, bf16), pltpu.VMEM(lq.shape, bf16),
            pltpu.VMEM(sq.shape, bf16), pltpu.VMEM((heads, toks), f32),
            pltpu.VMEM((heads, width), f32),
            pltpu.VMEM((n, toks, 2 * kv), bf16),
            pltpu.VMEM((width, toks), f32), pltpu.VMEM((heads, toks, width), f32),
            pltpu.VMEM((heads, toks), f32),
            pltpu.VMEM((heads, width, width), f32),
            pltpu.VMEM((heads, width, width), bf16), pltpu.VMEM((heads, width, width), bf16),
            pltpu.VMEM((toks, toks), f32), pltpu.VMEM((toks, toks), f32),
            pltpu.VMEM((heads, toks, width), f32),
            pltpu.VMEM((heads, width + 16, toks), f32), pltpu.VMEM((heads, 1, toks), f32),
            pltpu.VMEM((2 * toks, 2 * kv), bf16), pltpu.VMEM((2 * kv // width, toks // 2, width), f32),
            pltpu.VMEM((toks // 2, lq.shape[1]), bf16),
            dma((8,)), dma((n, PIECES)), dma((n, PIECES)), dma((heads,)), dma((heads,)), dma, dma,
        ],
        compiler_params=pltpu.CompilerParams(
            collective_id=0, has_side_effects=True, vmem_limit_bytes=58000000
        ),
        name="hybrid",
    )(lq, lk, lv, decay.T, gain.reshape(heads, width), sq, sk, sv, lengths)
    largest = jnp.finfo(bf16).max
    return tuple(jnp.minimum(x, largest) for x in (light, soft))


def solution(mesh):
    block = P(("groups", "seq"), ("section", "mp"))
    return jax.shard_map(
        functools.partial(body, mesh.shape["seq"]),
        mesh=mesh,
        in_specs=(block, block, block, block, P(("section", "mp")), block, block, block, P("groups")),
        out_specs=(block, block),
        check_vma=False,
    )
```

```python
import functools
import math

import jax
import jax.numpy as jnp
from jax import lax
from jax.experimental import pallas as pl
from jax.experimental.pallas import tpu as pltpu
from jax.sharding import PartitionSpec as P

MESH = pl.DeviceIdType.MESH
LOG2E = 1.4426950408889634
LOW = -1e30
CHUNK = 2
PIECES = 4
BATCH = 2
UNIT = 4
FINISH = 4


def mm(a, b, dims=((1,), (0,)), precision=None):
    return lax.dot_general(
        a, b, (dims, ((), ())), precision=precision, preferred_element_type=jnp.float32
    )


def can_pack(n, toks, width, heads, kv):
    return n == 4 and toks == 2 * width and heads >= 2 * kv // width


def kernel(
    n, width,
    lq_hbm, lk_hbm, lv_hbm, decay_hbm, gain_hbm, sq_hbm, sk_hbm, sv_hbm, lengths_hbm,
    light_out, soft_out,
    lengths, lq, lk, lv, sq, decay, gain, kvbuf,
    padded, cols, rows, states, state_in, state_out, bias, causal, insum, acc, peak, pack, spare, later_q,
    local_sem, kv_send, kv_recv, s_send, s_recv, q_send, q_recv,
):
    me = lax.axis_index("seq")
    right = {"seq": me + 1}
    heads, toks = decay.shape
    kv = kvbuf.shape[2] // 2
    kv_count = kv // width
    rows_piece = toks // PIECES
    half = toks // 2
    packed = can_pack(n, toks, width, heads, kv)
    tiles = 2 * kv // width
    last = n - 1
    group = heads // kv_count
    chunks = heads // CHUNK
    scale = width ** (-0.5)
    bf16, f32 = jnp.bfloat16, jnp.float32

    copies = [
        pltpu.make_async_copy(src, dst, local_sem.at[i])
        for i, (src, dst) in enumerate((
            (sk_hbm, kvbuf.at[0, :, :kv]), (sv_hbm, kvbuf.at[0, :, kv:]), (decay_hbm, decay), (lk_hbm, lk),
            (lv_hbm, lv), (sq_hbm, sq), (lq_hbm, lq), (gain_hbm, gain),
            (lengths_hbm, lengths),
        ))
    ]
    for copy in copies:
        copy.start()

    barrier = pltpu.get_barrier_semaphore()

    @pl.when(me > 0)
    def _():
        pl.semaphore_signal(barrier, inc=1, device_id={"seq": me - 1}, device_id_type=MESH)

    if packed:
        @pl.when(me == n - 2)
        def _():
            pl.semaphore_signal(barrier, inc=1, device_id=right, device_id_type=MESH)

    @pl.when(True if packed else me < n - 1)
    def _():
        pl.semaphore_wait(barrier, 1)

    def kv_copy(step, p):
        piece = pl.ds(p * rows_piece, rows_piece)
        return pltpu.make_async_remote_copy(
            src_ref=kvbuf.at[step, piece], dst_ref=kvbuf.at[step + 1, piece],
            send_sem=kv_send.at[step, p], recv_sem=kv_recv.at[step + 1, p],
            device_id=right, device_id_type=MESH,
        )

    def state_copy(b):
        batch = pl.ds(b * BATCH, BATCH)
        return pltpu.make_async_remote_copy(
            src_ref=state_out.at[batch], dst_ref=state_in.at[batch],
            send_sem=s_send.at[b], recv_sem=s_recv.at[b],
            device_id=right, device_id_type=MESH,
        )

    def pack_copy(k):
        step, p = divmod(k, PIECES)
        piece = pl.ds(p * rows_piece, rows_piece)
        return pltpu.make_async_remote_copy(
            src_ref=pack.at[pl.ds((k - PIECES // 2) * rows_piece, rows_piece)],
            dst_ref=kvbuf.at[step + 1, piece],
            send_sem=kv_send.at[step, p], recv_sem=kv_recv.at[step + 1, p],
            device_id=right, device_id_type=MESH,
        )

    query_copy = pltpu.make_async_remote_copy(
        src_ref=lq_hbm.at[:half], dst_ref=later_q, send_sem=q_send, recv_sem=q_recv,
        device_id={"seq": me - 1}, device_id_type=MESH,
    )
    packs = (me == n - 2) if packed else False
    unpacks = (me == last) if packed else False
    forwards = (me < n - 2) if packed else (me < last)

    if packed:
        @pl.when(unpacks)
        def _():
            query_copy.start()

    copies[0].wait()
    copies[1].wait()

    @pl.when(me < last)
    def _():
        for p in range(PIECES // 2):
            kv_copy(0, p).start()

    @pl.when(forwards)
    def _():
        for p in range(PIECES // 2, PIECES):
            kv_copy(0, p).start()

    copies[2].wait()
    copies[8].wait()
    own = lengths[me]
    if packed:
        ends = [lengths[b] for b in range(n)]
        short = ends[3] < half
        cut1 = jnp.where(short, ends[2] + ends[3] - toks, jnp.maximum(ends[2] - half, 0))
        cut0 = 2 * toks - ends[0]
    tok_col = lax.broadcasted_iota(jnp.int32, (toks, width), 0)
    live = tok_col < own
    padded[...] = jnp.zeros_like(padded)
    tok_lane = lax.broadcasted_iota(jnp.int32, (heads, toks), 1)
    masked = jnp.where(tok_lane < own, decay[...], 0.0)
    at0 = lax.broadcasted_iota(jnp.int32, (toks, toks), 0)
    at1 = lax.broadcasted_iota(jnp.int32, (toks, toks), 1)
    padded[:heads, :] = mm(masked, (at0 <= at1).astype(f32), precision=lax.Precision.HIGHEST)
    padded[:heads, :] = padded[:heads, :] * LOG2E
    rows[...] = padded[:heads, :]
    running = padded[...].T
    for h in range(heads):
        cols[h] = jnp.broadcast_to(running[:, h : h + 1], (toks, width))

    copies[3].wait()
    copies[4].wait()

    def head_lanes(h):
        return pl.ds(h * width if isinstance(h, int) else pl.multiple_of(h * width, width), width)

    def block_states(hs):
        faded = []
        for h in hs:
            col = cols[h]
            fading = jnp.where(live, jnp.exp2(col[toks - 1 : toks, :] - col), 0.0)
            faded.append((lk[:, head_lanes(h)].astype(f32) * fading).astype(bf16).T)
        found = [mm(x, lv[:, head_lanes(h)]) for h, x in zip(hs, faded)]
        for h, state in zip(hs, found):
            states[h] = state
            state_out[h] = state.astype(bf16)

    def insides(hs):
        parts = []
        for top in (True, False):
            size = half if top else toks
            span = slice(0, half) if top else slice(half, toks)
            raw = [mm(lq[span, head_lanes(h)], lk[:size, head_lanes(h)], ((1,), (1,))) for h in hs]
            weights = []
            for h, x in zip(hs, raw):
                wide = jnp.concatenate([cols[h, span, :]] * (size // width), axis=1)
                gaps = (wide - rows[h : h + 1, :size]) + causal[span, :size]
                weights.append((x * jnp.exp2(gaps)).astype(bf16))
            parts.append([mm(w, lv[:size, head_lanes(h)]) for h, w in zip(hs, weights)])
        for h, top, low in zip(hs, *parts):
            insum[h, :half, :] = top
            insum[h, half:, :] = low

    copies[5].wait()
    copies[6].wait()
    factor = scale * LOG2E
    bias[...] = jnp.where(at0 <= at1, 0.0, LOW)
    causal[...] = jnp.where(at0 >= at1, math.log2(scale), LOW)
    part = min(UNIT, group)
    units = heads // part
    pad = acc.shape[1] - width
    lane_pos = lax.broadcasted_iota(jnp.int32, (pad, toks), 1)

    def one_hot(size, span, shift, limit):
        dst = lax.broadcasted_iota(jnp.int32, (size, span), 0)
        src = lax.broadcasted_iota(jnp.int32, (size, span), 1)
        return jnp.where((src - dst == shift) & (src < limit), 1.0, 0.0).astype(bf16)

    def fill(j):
        start = j * rows_piece
        total = jnp.zeros((rows_piece, 2 * kv), f32)
        if start < half:
            at = lax.broadcasted_iota(jnp.int32, (rows_piece, 2 * kv), 0) + start
            tail = kvbuf[0, half + start : half + start + rows_piece, :].astype(f32)
            total = jnp.where(at < cut1, tail, total)
        low, high = max(0, start - half), min(toks, start + rows_piece)
        if low < high:
            hot = one_hot(rows_piece, high - low, start - low - cut1, ends[1] - low)
            total = total + mm(hot, kvbuf[1, low:high, :])
        if start >= toks:
            high = start - toks + rows_piece
            total = total + mm(one_hot(rows_piece, high, start - cut0, high), kvbuf[2, :high, :])
        pack[start : start + rows_piece, :] = total.astype(bf16)

    def arrive(step, u):
        each = PIECES // units
        for p in range(u * each, (u + 1) * each):
            needed = True if not packed else (me < last) | (step < last) | (p < PIECES // 2)

            @pl.when(needed)
            def _():
                kv_copy(step - 1, p).wait_recv()

            @pl.when(forwards)
            def _():
                kv_copy(step, p).start()

            if packed:
                for b in (1, 2) if not isinstance(step, int) else (step,):
                    @pl.when(packs & (step == b))
                    def _():
                        j = (b - 1) * PIECES + p
                        fill(j)
                        pack_copy(PIECES // 2 + j).start()

    def pass_states(b):
        hs = [b * BATCH + j for j in range(BATCH)]
        state_copy(b).wait_recv()
        kept = [jnp.exp2(cols[h, toks - 1 : toks, :]) for h in hs]
        left = [(k * state_in[h].astype(f32) + states[h]).astype(bf16) for h, k in zip(hs, kept)]
        for h, x in zip(hs, left):
            state_out[h] = x

        if packed:
            @pl.when(packs)
            def _():
                outs = [state_out[h] for h in hs]
                found = [mm(later_q[:, head_lanes(h)], x) for h, x in zip(hs, outs)]
                for h, x, y in zip(hs, outs, found):
                    extra = spare[jnp.minimum(h, tiles - 1)]
                    x = jnp.where(state_row < spare_end, extra, x.astype(f32))
                    state_out[h] = jnp.where(state_row < result_end, y, x).astype(bf16)

        state_copy(b).start()

    def unpack():
        for b in range(tiles // BATCH):
            state_copy(b).wait_recv()
        for h in range(tiles):
            kvbuf[last, half:, h * width : (h + 1) * width] = state_in[h]

    def ranges(step):
        if not packed:
            return lengths[me - step], toks, toks, toks
        flat = lengths[jnp.maximum(me - step, 0)]
        joint = cut1 + ends[1]
        at = [step == k for k in range(n)]

        def pick(plain, one, two, three):
            return jnp.where(unpacks, jnp.where(at[1], one, jnp.where(at[2], two, three)), plain)

        return (
            pick(flat, jnp.minimum(ends[2], half), joint - half, jnp.minimum(joint - toks - half, half)),
            pick(toks, half, toks, cut0 - toks - half),
            pick(toks, half + joint, toks, half),
            pick(toks, toks, cut0 - half, jnp.where(short, half + ends[3], toks)),
        )

    def within(at, limits):
        a, b, c, d = limits
        return (at < a) | ((at >= b) & (at < c)) | (at >= d)

    def attend(step, u, shared):
        first = isinstance(step, int)
        g, i = divmod(u, group // part)
        if i == 0:
            lanes_g = slice(g * width, (g + 1) * width)
            lanes_v = slice(kv + g * width, kv + (g + 1) * width)
            if first:
                keys = kvbuf[0, :, lanes_g]
                values = kvbuf[0, :, lanes_v].T
                counted = jnp.ones((pad, toks), bf16)
            else:
                limits = ranges(step)
                key_live = within(tok_col, limits)
                seen = kvbuf[0, 0:1, lanes_g].astype(f32)
                keys = kvbuf[step, :, lanes_g].astype(f32)
                keys = jnp.where(key_live, keys, seen).astype(bf16)
                values = kvbuf[step, :, lanes_v].astype(f32)
                values = jnp.where(key_live, values, 0.0).astype(bf16).T
                counted = jnp.where(within(lane_pos, limits), 1.0, 0.0).astype(bf16)
            shared[:] = [keys, jnp.concatenate([values, counted], axis=0)]
        keys, values = shared
        hs = [g * group + i * part + j for j in range(part)]
        scores = [mm(keys, sq[:, h * width : (h + 1) * width], ((1,), (1,))) for h in hs]
        if first:
            scores = [x + bias[...] for x in scores]
            peaks = [jnp.max(x, axis=0, keepdims=True) for x in scores]
        else:
            olds = [peak[h] for h in hs]
            peaks = [
                jnp.maximum(o, jnp.max(x, axis=0, keepdims=True)) for o, x in zip(olds, scores)
            ]
        probs = [jnp.exp2((x - p) * factor).astype(bf16) for x, p in zip(scores, peaks)]
        sums = [mm(values, x) for x in probs]
        if not first:
            sums = [
                jnp.exp2((o - p) * factor) * acc[h] + x
                for h, o, p, x in zip(hs, olds, peaks, sums)
            ]
        for h, p, x in zip(hs, peaks, sums):
            peak[h] = p
            acc[h] = x

    shared = []
    for u in range(units):
        @pl.when(me > 0)
        def _():
            arrive(1, u)

        attend(0, u, shared)
        hs = range(u * part, (u + 1) * part)
        block_states(hs)
        insides(hs)

        @pl.when(me == 0)
        def _():
            for b in range(u * part // BATCH, (u + 1) * part // BATCH):
                state_copy(b).start()

    if packed:
        state_row = lax.broadcasted_iota(jnp.int32, (width, width), 0)
        result_end = jnp.where(short, ends[3], 0)
        spare_end = jnp.where(short, width, 0)
        across_end = jnp.where(unpacks & short, half, 0)

    relays = (me > 0) & (me < last)
    early = heads // 2

    def later(step, carry):
        if packed:
            @pl.when(unpacks & (step == last))
            def _():
                unpack()

            @pl.when(packs & (step == me))
            def _():
                query_copy.wait_recv()
                moved = mm(one_hot(half, toks, ends[2] - half, toks), kvbuf[0])
                for h in range(tiles):
                    spare[h] = moved[:, h * width : (h + 1) * width]

        shared = []
        for u in range(units):
            @pl.when(step < me)
            def _():
                arrive(step + 1, u)

            @pl.when(relays & (step == me))
            def _():
                each = early // BATCH // units
                for b in range(u * each, (u + 1) * each):
                    pass_states(b)

            attend(step, u, shared)
        return carry

    lax.fori_loop(1, me + 1, later, 0)

    def finish_soft(c, carry):
        hs = [c * FINISH + j for j in range(FINISH)]
        results = [(acc[h, :width, :] / acc[h, width : width + 1, :]).T for h in hs]
        for h, x in zip(hs, results):
            soft_out[:, head_lanes(h)] = jnp.where(live, x, 0.0).astype(bf16)
        return carry

    lax.fori_loop(0, heads // FINISH, finish_soft, 0)

    copies[7].wait()

    @pl.when(me == 0)
    def _():
        state_in[...] = jnp.zeros_like(state_in)

    def lightning(c, carry):
        hs = [c * CHUNK + j for j in range(CHUNK)]

        @pl.when(relays & (c < chunks // 2))
        def _():
            for j in range(CHUNK // BATCH):
                pass_states((c * CHUNK + early) // BATCH + j)

        @pl.when((me == last) & (c >= tiles // CHUNK if packed else True))
        def _():
            for j in range(CHUNK // BATCH):
                state_copy(c * (CHUNK // BATCH) + j).wait_recv()

        across = [mm(lq[:, head_lanes(h)], state_in[h]) for h in hs]
        if packed:
            results = [state_in[h].astype(f32) for h in hs]
            results = [jnp.concatenate([x] * (toks // width), axis=0) for x in results]
            across = [jnp.where(tok_col < across_end, x, y) for x, y in zip(results, across)]
        drops = [jnp.exp2(cols[h]) * scale for h in hs]
        combined = [insum[h] + a * d for h, a, d in zip(hs, across, drops)]
        means = [jnp.mean(x * x, axis=1, keepdims=True) for x in combined]
        for h, x, mean in zip(hs, combined, means):
            normed = x * lax.rsqrt(mean + 1e-06) * gain[pl.ds(h, 1), :]
            light_out[:, head_lanes(h)] = jnp.where(live, normed, 0.0).astype(bf16)
        return carry

    lax.fori_loop(0, chunks, lightning, 0)

    if packed:
        @pl.when(unpacks)
        def _():
            query_copy.wait_send()

    @pl.when(me < n - 1)
    def _():
        def sent_blocks(step, carry):
            for p in range(PIECES):
                sent = True if not packed else (me < n - 2) | (step < n - 2) | (p < PIECES // 2)

                @pl.when(sent)
                def _():
                    kv_copy(step, p).wait_send()

            return carry

        lax.fori_loop(0, me + 1, sent_blocks, 0)

        def sent_states(b, carry):
            state_copy(b).wait_send()
            return carry

        lax.fori_loop(0, heads // BATCH, sent_states, 0)


def body(n, lq, lk, lv, decay, gain, sq, sk, sv, lengths):
    toks, heads = decay.shape
    width = lq.shape[1] // heads
    kv = sk.shape[1]
    chunks = heads // CHUNK
    bf16, f32 = jnp.bfloat16, jnp.float32
    out = pltpu.VMEM(lq.shape, bf16)
    dma = pltpu.SemaphoreType.DMA
    anywhere = pl.BlockSpec(memory_space=pltpu.HBM)
    vmem = pl.BlockSpec(memory_space=pltpu.VMEM)
    light, soft = pl.pallas_call(
        functools.partial(kernel, n, width),
        out_shape=(out, out),
        in_specs=[anywhere] * 9,
        out_specs=(vmem, vmem),
        scratch_shapes=[
            pltpu.SMEM(lengths.shape, lengths.dtype),
            pltpu.VMEM(lq.shape, bf16), pltpu.VMEM(lq.shape, bf16), pltpu.VMEM(lq.shape, bf16),
            pltpu.VMEM(sq.shape, bf16), pltpu.VMEM((heads, toks), f32),
            pltpu.VMEM((heads, width), f32),
            pltpu.VMEM((n, toks, 2 * kv), bf16),
            pltpu.VMEM((width, toks), f32), pltpu.VMEM((heads, toks, width), f32),
            pltpu.VMEM((heads, toks), f32),
            pltpu.VMEM((heads, width, width), f32),
            pltpu.VMEM((heads, width, width), bf16), pltpu.VMEM((heads, width, width), bf16),
            pltpu.VMEM((toks, toks), f32), pltpu.VMEM((toks, toks), f32),
            pltpu.VMEM((heads, toks, width), f32),
            pltpu.VMEM((heads, width + 16, toks), f32), pltpu.VMEM((heads, 1, toks), f32),
            pltpu.VMEM((2 * toks, 2 * kv), bf16), pltpu.VMEM((2 * kv // width, toks // 2, width), f32),
            pltpu.VMEM((toks // 2, lq.shape[1]), bf16),
            dma((9,)), dma((n, PIECES)), dma((n, PIECES)), dma((heads // BATCH,)), dma((heads // BATCH,)), dma, dma,
        ],
        compiler_params=pltpu.CompilerParams(
            collective_id=0, has_side_effects=True, vmem_limit_bytes=58000000
        ),
        name="hybrid",
    )(lq, lk, lv, decay.T, gain.reshape(heads, width), sq, sk, sv, lengths)
    largest = jnp.finfo(bf16).max
    return tuple(jnp.minimum(x, largest) for x in (light, soft))


def solution(mesh):
    block = P(("groups", "seq"), ("section", "mp"))
    return jax.shard_map(
        functools.partial(body, mesh.shape["seq"]),
        mesh=mesh,
        in_specs=(block, block, block, block, P(("section", "mp")), block, block, block, P("groups")),
        out_specs=(block, block),
        check_vma=False,
    )
```

```python
import functools
import math

import jax
import jax.numpy as jnp
from jax import lax
from jax.experimental import pallas as pl
from jax.experimental.pallas import tpu as pltpu
from jax.sharding import PartitionSpec as P

MESH = pl.DeviceIdType.MESH
LOG2E = 1.4426950408889634
LOW = -1e30
CHUNK = 2
PIECES = 4
BATCH = 2
UNIT = 4
FINISH = 4


def mm(a, b, dims=((1,), (0,)), precision=None):
    return lax.dot_general(
        a, b, (dims, ((), ())), precision=precision, preferred_element_type=jnp.float32
    )


def can_pack(n, toks, width, heads, kv):
    return n == 4 and toks == 2 * width and heads >= 2 * kv // width


def kernel(
    n, width,
    lq_hbm, lk_hbm, lv_hbm, decay_hbm, gain_hbm, sq_hbm, sk_hbm, sv_hbm, lengths_hbm,
    light_out, soft_out, end_q, end_state, end_sum, end_drop, end_mask, end_gain,
    lengths, lq, lk, lv, sq, decay, gain, kvbuf,
    padded, cols, rows, states, state_in, state_out, bias, causal, insum, acc, peak, pack, spare, later_q,
    local_sem, kv_send, kv_recv, s_send, s_recv, q_send, q_recv,
):
    me = lax.axis_index("seq")
    right = {"seq": me + 1}
    heads, toks = decay.shape
    kv = kvbuf.shape[2] // 2
    kv_count = kv // width
    rows_piece = toks // PIECES
    half = toks // 2
    packed = can_pack(n, toks, width, heads, kv)
    tiles = 2 * kv // width
    last = n - 1
    group = heads // kv_count
    chunks = heads // CHUNK
    scale = width ** (-0.5)
    bf16, f32 = jnp.bfloat16, jnp.float32

    copies = [
        pltpu.make_async_copy(src, dst, local_sem.at[i])
        for i, (src, dst) in enumerate((
            (sk_hbm, kvbuf.at[0, :, :kv]), (sv_hbm, kvbuf.at[0, :, kv:]), (decay_hbm, decay), (lk_hbm, lk),
            (lv_hbm, lv), (sq_hbm, sq), (lq_hbm, lq), (gain_hbm, gain),
            (lengths_hbm, lengths),
        ))
    ]
    for copy in copies:
        copy.start()

    barrier = pltpu.get_barrier_semaphore()

    @pl.when(me > 0)
    def _():
        pl.semaphore_signal(barrier, inc=1, device_id={"seq": me - 1}, device_id_type=MESH)

    if packed:
        @pl.when(me == n - 2)
        def _():
            pl.semaphore_signal(barrier, inc=1, device_id=right, device_id_type=MESH)

    @pl.when(True if packed else me < n - 1)
    def _():
        pl.semaphore_wait(barrier, 1)

    def kv_copy(step, p):
        piece = pl.ds(p * rows_piece, rows_piece)
        return pltpu.make_async_remote_copy(
            src_ref=kvbuf.at[step, piece], dst_ref=kvbuf.at[step + 1, piece],
            send_sem=kv_send.at[step, p], recv_sem=kv_recv.at[step + 1, p],
            device_id=right, device_id_type=MESH,
        )

    def state_copy(b):
        batch = pl.ds(b * BATCH, BATCH)
        return pltpu.make_async_remote_copy(
            src_ref=state_out.at[batch], dst_ref=state_in.at[batch],
            send_sem=s_send.at[b], recv_sem=s_recv.at[b],
            device_id=right, device_id_type=MESH,
        )

    def pack_copy(k):
        step, p = divmod(k, PIECES)
        piece = pl.ds(p * rows_piece, rows_piece)
        return pltpu.make_async_remote_copy(
            src_ref=pack.at[pl.ds((k - PIECES // 2) * rows_piece, rows_piece)],
            dst_ref=kvbuf.at[step + 1, piece],
            send_sem=kv_send.at[step, p], recv_sem=kv_recv.at[step + 1, p],
            device_id=right, device_id_type=MESH,
        )

    query_copy = pltpu.make_async_remote_copy(
        src_ref=lq_hbm.at[:half], dst_ref=later_q, send_sem=q_send, recv_sem=q_recv,
        device_id={"seq": me - 1}, device_id_type=MESH,
    )
    packs = (me == n - 2) if packed else False
    unpacks = (me == last) if packed else False
    forwards = (me < n - 2) if packed else (me < last)

    if packed:
        @pl.when(unpacks)
        def _():
            query_copy.start()

    copies[0].wait()
    copies[1].wait()

    @pl.when(me < last)
    def _():
        for p in range(PIECES // 2):
            kv_copy(0, p).start()

    @pl.when(forwards)
    def _():
        for p in range(PIECES // 2, PIECES):
            kv_copy(0, p).start()

    copies[2].wait()
    copies[8].wait()
    own = lengths[me]
    if packed:
        ends = [lengths[b] for b in range(n)]
        short = ends[3] < half
        cut1 = jnp.where(short, ends[2] + ends[3] - toks, jnp.maximum(ends[2] - half, 0))
        cut0 = 2 * toks - ends[0]
    tok_col = lax.broadcasted_iota(jnp.int32, (toks, width), 0)
    live = tok_col < own
    padded[...] = jnp.zeros_like(padded)
    tok_lane = lax.broadcasted_iota(jnp.int32, (heads, toks), 1)
    masked = jnp.where(tok_lane < own, decay[...], 0.0)
    at0 = lax.broadcasted_iota(jnp.int32, (toks, toks), 0)
    at1 = lax.broadcasted_iota(jnp.int32, (toks, toks), 1)
    padded[:heads, :] = mm(masked, (at0 <= at1).astype(f32), precision=lax.Precision.HIGHEST)
    padded[:heads, :] = padded[:heads, :] * LOG2E
    rows[...] = padded[:heads, :]
    running = padded[...].T
    for h in range(heads):
        cols[h] = jnp.broadcast_to(running[:, h : h + 1], (toks, width))

    copies[3].wait()
    copies[4].wait()

    def head_lanes(h):
        return pl.ds(h * width if isinstance(h, int) else pl.multiple_of(h * width, width), width)

    def block_states(hs):
        faded = []
        for h in hs:
            col = cols[h]
            fading = jnp.where(live, jnp.exp2(col[toks - 1 : toks, :] - col), 0.0)
            faded.append((lk[:, head_lanes(h)].astype(f32) * fading).astype(bf16).T)
        found = [mm(x, lv[:, head_lanes(h)]) for h, x in zip(hs, faded)]
        for h, state in zip(hs, found):
            states[h] = state
            state_out[h] = state.astype(bf16)

    def insides(hs):
        parts = []
        for top in (True, False):
            size = half if top else toks
            span = slice(0, half) if top else slice(half, toks)
            raw = [mm(lq[span, head_lanes(h)], lk[:size, head_lanes(h)], ((1,), (1,))) for h in hs]
            weights = []
            for h, x in zip(hs, raw):
                wide = jnp.concatenate([cols[h, span, :]] * (size // width), axis=1)
                gaps = (wide - rows[h : h + 1, :size]) + causal[span, :size]
                weights.append((x * jnp.exp2(gaps)).astype(bf16))
            parts.append([mm(w, lv[:size, head_lanes(h)]) for h, w in zip(hs, weights)])
        for h, top, low in zip(hs, *parts):
            insum[h, :half, :] = top
            insum[h, half:, :] = low

    copies[5].wait()
    copies[6].wait()
    factor = scale * LOG2E
    bias[...] = jnp.where(at0 <= at1, 0.0, LOW)
    causal[...] = jnp.where(at0 >= at1, math.log2(scale), LOW)
    part = min(UNIT, group)
    units = heads // part
    pad = acc.shape[1] - width
    lane_pos = lax.broadcasted_iota(jnp.int32, (pad, toks), 1)

    def one_hot(size, span, shift, limit):
        dst = lax.broadcasted_iota(jnp.int32, (size, span), 0)
        src = lax.broadcasted_iota(jnp.int32, (size, span), 1)
        return jnp.where((src - dst == shift) & (src < limit), 1.0, 0.0).astype(bf16)

    def fill(j):
        start = j * rows_piece
        total = jnp.zeros((rows_piece, 2 * kv), f32)
        if start < half:
            at = lax.broadcasted_iota(jnp.int32, (rows_piece, 2 * kv), 0) + start
            tail = kvbuf[0, half + start : half + start + rows_piece, :].astype(f32)
            total = jnp.where(at < cut1, tail, total)
        low, high = max(0, start - half), min(toks, start + rows_piece)
        if low < high:
            hot = one_hot(rows_piece, high - low, start - low - cut1, ends[1] - low)
            total = total + mm(hot, kvbuf[1, low:high, :])
        if start >= toks:
            high = start - toks + rows_piece
            total = total + mm(one_hot(rows_piece, high, start - cut0, high), kvbuf[2, :high, :])
        pack[start : start + rows_piece, :] = total.astype(bf16)

    def arrive(step, u):
        each = PIECES // units
        for p in range(u * each, (u + 1) * each):
            needed = True if not packed else (me < last) | (step < last) | (p < PIECES // 2)

            @pl.when(needed)
            def _():
                kv_copy(step - 1, p).wait_recv()

            @pl.when(forwards)
            def _():
                kv_copy(step, p).start()

            if packed:
                for b in (1, 2) if not isinstance(step, int) else (step,):
                    @pl.when(packs & (step == b))
                    def _():
                        j = (b - 1) * PIECES + p
                        fill(j)
                        pack_copy(PIECES // 2 + j).start()

    def pass_states(b):
        hs = [b * BATCH + j for j in range(BATCH)]
        state_copy(b).wait_recv()
        kept = [jnp.exp2(cols[h, toks - 1 : toks, :]) for h in hs]
        left = [(k * state_in[h].astype(f32) + states[h]).astype(bf16) for h, k in zip(hs, kept)]
        for h, x in zip(hs, left):
            state_out[h] = x

        if packed:
            @pl.when(packs)
            def _():
                outs = [state_out[h] for h in hs]
                found = [mm(later_q[:, head_lanes(h)], x) for h, x in zip(hs, outs)]
                for h, x, y in zip(hs, outs, found):
                    extra = spare[jnp.minimum(h, tiles - 1)]
                    x = jnp.where(state_row < spare_end, extra, x.astype(f32))
                    state_out[h] = jnp.where(state_row < result_end, y, x).astype(bf16)

        state_copy(b).start()

    def unpack():
        for b in range(tiles // BATCH):
            state_copy(b).wait_recv()
        for h in range(tiles):
            kvbuf[last, half:, h * width : (h + 1) * width] = state_in[h]

    def ranges(step):
        if not packed:
            return lengths[me - step], toks, toks, toks
        flat = lengths[jnp.maximum(me - step, 0)]
        joint = cut1 + ends[1]
        at = [step == k for k in range(n)]

        def pick(plain, one, two, three):
            return jnp.where(unpacks, jnp.where(at[1], one, jnp.where(at[2], two, three)), plain)

        return (
            pick(flat, jnp.minimum(ends[2], half), joint - half, jnp.minimum(joint - toks - half, half)),
            pick(toks, half, toks, cut0 - toks - half),
            pick(toks, half + joint, toks, half),
            pick(toks, toks, cut0 - half, jnp.where(short, half + ends[3], toks)),
        )

    def within(at, limits):
        a, b, c, d = limits
        return (at < a) | ((at >= b) & (at < c)) | (at >= d)

    def attend(step, u, shared):
        first = isinstance(step, int)
        g, i = divmod(u, group // part)
        if i == 0:
            lanes_g = slice(g * width, (g + 1) * width)
            lanes_v = slice(kv + g * width, kv + (g + 1) * width)
            if first:
                keys = kvbuf[0, :, lanes_g]
                values = kvbuf[0, :, lanes_v].T
                counted = jnp.ones((pad, toks), bf16)
            else:
                limits = ranges(step)
                key_live = within(tok_col, limits)
                seen = kvbuf[0, 0:1, lanes_g].astype(f32)
                keys = kvbuf[step, :, lanes_g].astype(f32)
                keys = jnp.where(key_live, keys, seen).astype(bf16)
                values = kvbuf[step, :, lanes_v].astype(f32)
                values = jnp.where(key_live, values, 0.0).astype(bf16).T
                counted = jnp.where(within(lane_pos, limits), 1.0, 0.0).astype(bf16)
            shared[:] = [keys, jnp.concatenate([values, counted], axis=0)]
        keys, values = shared
        hs = [g * group + i * part + j for j in range(part)]
        scores = [mm(keys, sq[:, h * width : (h + 1) * width], ((1,), (1,))) for h in hs]
        if first:
            scores = [x + bias[...] for x in scores]
            peaks = [jnp.max(x, axis=0, keepdims=True) for x in scores]
        else:
            olds = [peak[h] for h in hs]
            peaks = [
                jnp.maximum(o, jnp.max(x, axis=0, keepdims=True)) for o, x in zip(olds, scores)
            ]
        probs = [jnp.exp2((x - p) * factor).astype(bf16) for x, p in zip(scores, peaks)]
        sums = [mm(values, x) for x in probs]
        if not first:
            sums = [
                jnp.exp2((o - p) * factor) * acc[h] + x
                for h, o, p, x in zip(hs, olds, peaks, sums)
            ]
        for h, p, x in zip(hs, peaks, sums):
            peak[h] = p
            acc[h] = x

    shared = []
    for u in range(units):
        @pl.when(me > 0)
        def _():
            arrive(1, u)

        attend(0, u, shared)
        hs = range(u * part, (u + 1) * part)
        block_states(hs)
        insides(hs)

        @pl.when(me == 0)
        def _():
            for b in range(u * part // BATCH, (u + 1) * part // BATCH):
                state_copy(b).start()

    if packed:
        state_row = lax.broadcasted_iota(jnp.int32, (width, width), 0)
        result_end = jnp.where(short, ends[3], 0)
        spare_end = jnp.where(short, width, 0)
        across_end = jnp.where(unpacks & short, half, 0)

    relays = (me > 0) & (me < last)
    early = heads // 2

    def later(step, carry):
        if packed:
            @pl.when(unpacks & (step == last))
            def _():
                unpack()

            @pl.when(packs & (step == me))
            def _():
                query_copy.wait_recv()
                moved = mm(one_hot(half, toks, ends[2] - half, toks), kvbuf[0])
                for h in range(tiles):
                    spare[h] = moved[:, h * width : (h + 1) * width]

        shared = []
        for u in range(units):
            @pl.when(step < me)
            def _():
                arrive(step + 1, u)

            @pl.when(relays & (step == me))
            def _():
                each = early // BATCH // units
                for b in range(u * each, (u + 1) * each):
                    pass_states(b)

            attend(step, u, shared)
        return carry

    lax.fori_loop(1, me + 1, later, 0)

    def finish_soft(c, carry):
        hs = [c * FINISH + j for j in range(FINISH)]
        results = [(acc[h, :width, :] / acc[h, width : width + 1, :]).T for h in hs]
        for h, x in zip(hs, results):
            soft_out[:, head_lanes(h)] = jnp.where(live, x, 0.0).astype(bf16)
        return carry

    lax.fori_loop(0, heads // FINISH, finish_soft, 0)

    copies[7].wait()

    @pl.when(me == 0)
    def _():
        state_in[...] = jnp.zeros_like(state_in)

    ends_at = heads - CHUNK
    end_q[...] = lq[:, ends_at * width :]
    for j in range(CHUNK):
        end_sum[j] = insum[ends_at + j]
        end_drop[j] = jnp.exp2(cols[ends_at + j]) * scale
    end_gain[...] = gain[ends_at:, :]
    mask = jnp.where(live, 1.0, 0.0)
    end_mask[...] = jnp.where(tok_col < across_end, mask + 2.0, mask) if packed else mask

    def lightning(c, carry):
        hs = [c * CHUNK + j for j in range(CHUNK)]

        @pl.when(relays & (c < chunks // 2))
        def _():
            for j in range(CHUNK // BATCH):
                pass_states((c * CHUNK + early) // BATCH + j)

        @pl.when((me == last) & (c >= tiles // CHUNK if packed else True))
        def _():
            for j in range(CHUNK // BATCH):
                state_copy(c * (CHUNK // BATCH) + j).wait_recv()

        across = [mm(lq[:, head_lanes(h)], state_in[h]) for h in hs]
        if packed:
            results = [state_in[h].astype(f32) for h in hs]
            results = [jnp.concatenate([x] * (toks // width), axis=0) for x in results]
            across = [jnp.where(tok_col < across_end, x, y) for x, y in zip(results, across)]
        drops = [jnp.exp2(cols[h]) * scale for h in hs]
        combined = [insum[h] + a * d for h, a, d in zip(hs, across, drops)]
        means = [jnp.mean(x * x, axis=1, keepdims=True) for x in combined]
        for h, x, mean in zip(hs, combined, means):
            normed = x * lax.rsqrt(mean + 1e-06) * gain[pl.ds(h, 1), :]
            light_out[:, head_lanes(h)] = jnp.where(live, normed, 0.0).astype(bf16)
        return carry

    lax.fori_loop(0, chunks - 1, lightning, 0)

    @pl.when(me == last)
    def _():
        for j in range(CHUNK // BATCH):
            state_copy(ends_at // BATCH + j).wait_recv()

    for j in range(CHUNK):
        end_state[j] = state_in[ends_at + j]

    if packed:
        @pl.when(unpacks)
        def _():
            query_copy.wait_send()

    @pl.when(me < n - 1)
    def _():
        def sent_blocks(step, carry):
            for p in range(PIECES):
                sent = True if not packed else (me < n - 2) | (step < n - 2) | (p < PIECES // 2)

                @pl.when(sent)
                def _():
                    kv_copy(step, p).wait_send()

            return carry

        lax.fori_loop(0, me + 1, sent_blocks, 0)

        def sent_states(b, carry):
            state_copy(b).wait_send()
            return carry

        lax.fori_loop(0, heads // BATCH, sent_states, 0)


def finish(
    light, soft, end_q, end_state, end_sum, end_drop, end_mask, end_gain,
    light_hbm, soft_hbm, ready, sem,
):
    toks, width = end_mask.shape
    done = light.shape[1] - end_q.shape[1]
    f32 = jnp.float32
    copies = [
        pltpu.make_async_copy(soft, soft_hbm, sem.at[0]),
        pltpu.make_async_copy(light.at[:, :done], light_hbm.at[:, :done], sem.at[1]),
        pltpu.make_async_copy(ready, light_hbm.at[:, done:], sem.at[2]),
    ]
    copies[0].start()
    copies[1].start()
    mask = end_mask[...]
    spans = [slice(j * width, (j + 1) * width) for j in range(CHUNK)]
    across = [mm(end_q[:, span], end_state[j]) for j, span in enumerate(spans)]
    given = [end_state[j].astype(f32) for j in range(CHUNK)]
    given = [jnp.concatenate([x] * (toks // width), axis=0) for x in given]
    across = [jnp.where(mask > 1.5, x, y) for x, y in zip(given, across)]
    combined = [end_sum[j] + x * end_drop[j] for j, x in enumerate(across)]
    means = [jnp.mean(x * x, axis=1, keepdims=True) for x in combined]
    live = (mask == 1.0) | (mask == 3.0)
    for j, (x, mean) in enumerate(zip(combined, means)):
        normed = x * lax.rsqrt(mean + 1e-06) * end_gain[j : j + 1, :]
        ready[:, spans[j]] = jnp.where(live, normed, 0.0).astype(jnp.bfloat16)
    copies[2].start()
    for copy in copies:
        copy.wait()


def body(n, lq, lk, lv, decay, gain, sq, sk, sv, lengths):
    toks, heads = decay.shape
    width = lq.shape[1] // heads
    kv = sk.shape[1]
    chunks = heads // CHUNK
    bf16, f32 = jnp.bfloat16, jnp.float32
    out = pltpu.VMEM(lq.shape, bf16)
    dma = pltpu.SemaphoreType.DMA
    anywhere = pl.BlockSpec(memory_space=pltpu.HBM)
    vmem = pl.BlockSpec(memory_space=pltpu.VMEM)
    ends = CHUNK * width
    left = pl.pallas_call(
        functools.partial(kernel, n, width),
        out_shape=(
            out, out, pltpu.VMEM((toks, ends), bf16), pltpu.VMEM((CHUNK, width, width), bf16),
            pltpu.VMEM((CHUNK, toks, width), f32), pltpu.VMEM((CHUNK, toks, width), f32),
            pltpu.VMEM((toks, width), f32), pltpu.VMEM((CHUNK, width), f32),
        ),
        in_specs=[anywhere] * 9,
        out_specs=(vmem,) * 8,
        scratch_shapes=[
            pltpu.SMEM(lengths.shape, lengths.dtype),
            pltpu.VMEM(lq.shape, bf16), pltpu.VMEM(lq.shape, bf16), pltpu.VMEM(lq.shape, bf16),
            pltpu.VMEM(sq.shape, bf16), pltpu.VMEM((heads, toks), f32),
            pltpu.VMEM((heads, width), f32),
            pltpu.VMEM((n, toks, 2 * kv), bf16),
            pltpu.VMEM((width, toks), f32), pltpu.VMEM((heads, toks, width), f32),
            pltpu.VMEM((heads, toks), f32),
            pltpu.VMEM((heads, width, width), f32),
            pltpu.VMEM((heads, width, width), bf16), pltpu.VMEM((heads, width, width), bf16),
            pltpu.VMEM((toks, toks), f32), pltpu.VMEM((toks, toks), f32),
            pltpu.VMEM((heads, toks, width), f32),
            pltpu.VMEM((heads, width + 16, toks), f32), pltpu.VMEM((heads, 1, toks), f32),
            pltpu.VMEM((2 * toks, 2 * kv), bf16), pltpu.VMEM((2 * kv // width, toks // 2, width), f32),
            pltpu.VMEM((toks // 2, lq.shape[1]), bf16),
            dma((9,)), dma((n, PIECES)), dma((n, PIECES)), dma((heads // BATCH,)), dma((heads // BATCH,)), dma, dma,
        ],
        compiler_params=pltpu.CompilerParams(
            collective_id=0, has_side_effects=True, vmem_limit_bytes=58000000
        ),
        name="hybrid",
    )(lq, lk, lv, decay.T, gain.reshape(heads, width), sq, sk, sv, lengths)
    whole = jax.ShapeDtypeStruct(lq.shape, bf16)
    return pl.pallas_call(
        finish,
        out_shape=(whole, whole),
        in_specs=[vmem] * 8,
        out_specs=(anywhere, anywhere),
        scratch_shapes=[pltpu.VMEM((toks, ends), bf16), dma((3,))],
        compiler_params=pltpu.CompilerParams(vmem_limit_bytes=4000000),
        name="finish",
    )(*left)


def solution(mesh):
    block = P(("groups", "seq"), ("section", "mp"))
    return jax.shard_map(
        functools.partial(body, mesh.shape["seq"]),
        mesh=mesh,
        in_specs=(block, block, block, block, P(("section", "mp")), block, block, block, P("groups")),
        out_specs=(block, block),
        check_vma=False,
    )
```

```python
import functools
import math

import jax
import jax.numpy as jnp
from jax import lax
from jax.experimental import pallas as pl
from jax.experimental.pallas import tpu as pltpu
from jax.sharding import PartitionSpec as P

MESH = pl.DeviceIdType.MESH
LOG2E = 1.4426950408889634
LOW = -1e30
CHUNK = 2
PIECES = 4
BATCH = 2
UNIT = 4
FINISH = 4


def mm(a, b, dims=((1,), (0,)), precision=None):
    return lax.dot_general(
        a, b, (dims, ((), ())), precision=precision, preferred_element_type=jnp.float32
    )


def can_pack(n, toks, width, heads, kv):
    return n == 4 and toks == 2 * width and heads >= 2 * kv // width


def kernel(
    n, width,
    lq_hbm, lk_hbm, lv_hbm, decay_hbm, gain_hbm, sq_hbm, sk_hbm, sv_hbm, lengths_hbm,
    light_out, soft_out, end_q, end_state, end_sum, end_drop, end_mask, end_gain,
    lengths, lq, lk, lv, sq, decay, gain, kvbuf,
    padded, cols, rows, states, state_in, state_out, bias, causal, insum, acc, peak, pack, spare, later_q,
    local_sem, kv_send, kv_recv, s_send, s_recv, q_send, q_recv,
):
    me = lax.axis_index("seq")
    right = {"seq": me + 1}
    heads, toks = decay.shape
    kv = kvbuf.shape[2] // 2
    kv_count = kv // width
    rows_piece = toks // PIECES
    half = toks // 2
    packed = can_pack(n, toks, width, heads, kv)
    tiles = 2 * kv // width
    last = n - 1
    group = heads // kv_count
    chunks = heads // CHUNK
    scale = width ** (-0.5)
    bf16, f32 = jnp.bfloat16, jnp.float32

    barrier = pltpu.get_barrier_semaphore()

    @pl.when(me > 0)
    def _():
        pl.semaphore_signal(barrier, inc=1, device_id={"seq": me - 1}, device_id_type=MESH)

    if packed:
        @pl.when(me == n - 2)
        def _():
            pl.semaphore_signal(barrier, inc=1, device_id=right, device_id_type=MESH)

    copies = [
        pltpu.make_async_copy(src, dst, local_sem.at[i])
        for i, (src, dst) in enumerate((
            (sk_hbm, kvbuf.at[0, :, :kv]), (sv_hbm, kvbuf.at[0, :, kv:]), (decay_hbm, decay), (lk_hbm, lk),
            (lv_hbm, lv), (sq_hbm, sq), (lq_hbm, lq), (gain_hbm, gain),
            (lengths_hbm, lengths),
        ))
    ]
    for copy in (copies[0], copies[1], copies[2], copies[8]):
        copy.start()

    @pl.when(True if packed else me < n - 1)
    def _():
        pl.semaphore_wait(barrier, 1)

    def kv_copy(step, p):
        piece = pl.ds(p * rows_piece, rows_piece)
        return pltpu.make_async_remote_copy(
            src_ref=kvbuf.at[step, piece], dst_ref=kvbuf.at[step + 1, piece],
            send_sem=kv_send.at[step, p], recv_sem=kv_recv.at[step + 1, p],
            device_id=right, device_id_type=MESH,
        )

    def state_copy(b):
        batch = pl.ds(b * BATCH, BATCH)
        return pltpu.make_async_remote_copy(
            src_ref=state_out.at[batch], dst_ref=state_in.at[batch],
            send_sem=s_send.at[b], recv_sem=s_recv.at[b],
            device_id=right, device_id_type=MESH,
        )

    def pack_copy(k):
        step, p = divmod(k, PIECES)
        piece = pl.ds(p * rows_piece, rows_piece)
        return pltpu.make_async_remote_copy(
            src_ref=pack.at[pl.ds((k - PIECES // 2) * rows_piece, rows_piece)],
            dst_ref=kvbuf.at[step + 1, piece],
            send_sem=kv_send.at[step, p], recv_sem=kv_recv.at[step + 1, p],
            device_id=right, device_id_type=MESH,
        )

    front_copy = pltpu.make_async_remote_copy(
        src_ref=kvbuf.at[0, :half], dst_ref=kvbuf.at[1, :half],
        send_sem=kv_send.at[0, 0], recv_sem=kv_recv.at[1, 0],
        device_id=right, device_id_type=MESH,
    )
    query_copy = pltpu.make_async_remote_copy(
        src_ref=lq_hbm.at[:half], dst_ref=later_q, send_sem=q_send, recv_sem=q_recv,
        device_id={"seq": me - 1}, device_id_type=MESH,
    )
    packs = (me == n - 2) if packed else False
    unpacks = (me == last) if packed else False
    forwards = (me < n - 2) if packed else (me < last)

    if packed:
        @pl.when(unpacks)
        def _():
            query_copy.start()

    copies[0].wait()
    copies[1].wait()

    if packed:
        @pl.when(packs)
        def _():
            front_copy.start()

    @pl.when(forwards)
    def _():
        for p in range(PIECES):
            kv_copy(0, p).start()

    for copy in copies[3:8]:
        copy.start()

    copies[2].wait()
    copies[8].wait()
    own = lengths[me]
    if packed:
        ends = [lengths[b] for b in range(n)]
        short = ends[3] < half
        cut1 = jnp.where(short, ends[2] + ends[3] - toks, jnp.maximum(ends[2] - half, 0))
        cut0 = 2 * toks - ends[0]
    tok_col = lax.broadcasted_iota(jnp.int32, (toks, width), 0)
    live = tok_col < own
    padded[...] = jnp.zeros_like(padded)
    tok_lane = lax.broadcasted_iota(jnp.int32, (heads, toks), 1)
    masked = jnp.where(tok_lane < own, decay[...], 0.0)
    at0 = lax.broadcasted_iota(jnp.int32, (toks, toks), 0)
    at1 = lax.broadcasted_iota(jnp.int32, (toks, toks), 1)
    padded[:heads, :] = mm(masked, (at0 <= at1).astype(f32), precision=lax.Precision.HIGHEST)
    padded[:heads, :] = padded[:heads, :] * LOG2E
    rows[...] = padded[:heads, :]
    running = padded[...].T
    for h in range(heads):
        cols[h] = jnp.broadcast_to(running[:, h : h + 1], (toks, width))

    copies[3].wait()
    copies[4].wait()

    def head_lanes(h):
        return pl.ds(h * width if isinstance(h, int) else pl.multiple_of(h * width, width), width)

    def block_states(hs):
        faded = []
        for h in hs:
            col = cols[h]
            fading = jnp.where(live, jnp.exp2(col[toks - 1 : toks, :] - col), 0.0)
            faded.append((lk[:, head_lanes(h)].astype(f32) * fading).astype(bf16).T)
        found = [mm(x, lv[:, head_lanes(h)]) for h, x in zip(hs, faded)]
        for h, state in zip(hs, found):
            states[h] = state
            state_out[h] = state.astype(bf16)

    def insides(hs):
        parts = []
        for top in (True, False):
            size = half if top else toks
            span = slice(0, half) if top else slice(half, toks)
            raw = [mm(lq[span, head_lanes(h)], lk[:size, head_lanes(h)], ((1,), (1,))) for h in hs]
            weights = []
            for h, x in zip(hs, raw):
                wide = jnp.concatenate([cols[h, span, :]] * (size // width), axis=1)
                gaps = (wide - rows[h : h + 1, :size]) + causal[span, :size]
                weights.append((x * jnp.exp2(gaps)).astype(bf16))
            parts.append([mm(w, lv[:size, head_lanes(h)]) for h, w in zip(hs, weights)])
        for h, top, low in zip(hs, *parts):
            insum[h, :half, :] = top
            insum[h, half:, :] = low

    copies[5].wait()
    copies[6].wait()
    factor = scale * LOG2E
    bias[...] = jnp.where(at0 <= at1, 0.0, LOW)
    causal[...] = jnp.where(at0 >= at1, math.log2(scale), LOW)
    part = min(UNIT, group)
    units = heads // part
    pad = acc.shape[1] - width
    lane_pos = lax.broadcasted_iota(jnp.int32, (pad, toks), 1)

    def one_hot(size, span, shift, limit):
        dst = lax.broadcasted_iota(jnp.int32, (size, span), 0)
        src = lax.broadcasted_iota(jnp.int32, (size, span), 1)
        return jnp.where((src - dst == shift) & (src < limit), 1.0, 0.0).astype(bf16)

    def fill(j):
        start = j * rows_piece
        total = jnp.zeros((rows_piece, 2 * kv), f32)
        if start < half:
            at = lax.broadcasted_iota(jnp.int32, (rows_piece, 2 * kv), 0) + start
            tail = kvbuf[0, half + start : half + start + rows_piece, :].astype(f32)
            total = jnp.where(at < cut1, tail, total)
        low, high = max(0, start - half), min(toks, start + rows_piece)
        if low < high:
            hot = one_hot(rows_piece, high - low, start - low - cut1, ends[1] - low)
            total = total + mm(hot, kvbuf[1, low:high, :])
        if start >= toks:
            high = start - toks + rows_piece
            total = total + mm(one_hot(rows_piece, high, start - cut0, high), kvbuf[2, :high, :])
        pack[start : start + rows_piece, :] = total.astype(bf16)

    def arrive(step, u):
        each = PIECES // units
        for p in range(u * each, (u + 1) * each):
            needed = True if not packed else (me < last) | (step < last) | (p < PIECES // 2)
            if packed and isinstance(step, int) and p < PIECES // 2:
                needed = me < last
                if p == 0:
                    @pl.when(unpacks)
                    def _():
                        front_copy.wait_recv()

            @pl.when(needed)
            def _():
                kv_copy(step - 1, p).wait_recv()

            @pl.when(forwards)
            def _():
                kv_copy(step, p).start()

            if packed:
                for b in (1, 2) if not isinstance(step, int) else (step,):
                    @pl.when(packs & (step == b))
                    def _():
                        j = (b - 1) * PIECES + p
                        fill(j)
                        pack_copy(PIECES // 2 + j).start()

    def pass_states(b):
        hs = [b * BATCH + j for j in range(BATCH)]
        state_copy(b).wait_recv()
        kept = [jnp.exp2(cols[h, toks - 1 : toks, :]) for h in hs]
        left = [(k * state_in[h].astype(f32) + states[h]).astype(bf16) for h, k in zip(hs, kept)]
        for h, x in zip(hs, left):
            state_out[h] = x

        if packed:
            @pl.when(packs)
            def _():
                outs = [state_out[h] for h in hs]
                found = [mm(later_q[:, head_lanes(h)], x) for h, x in zip(hs, outs)]
                for h, x, y in zip(hs, outs, found):
                    extra = spare[jnp.minimum(h, tiles - 1)]
                    x = jnp.where(state_row < spare_end, extra, x.astype(f32))
                    state_out[h] = jnp.where(state_row < result_end, y, x).astype(bf16)

        state_copy(b).start()

    def unpack():
        for b in range(tiles // BATCH):
            state_copy(b).wait_recv()
        for h in range(tiles):
            kvbuf[last, half:, h * width : (h + 1) * width] = state_in[h]

    def ranges(step):
        if not packed:
            return lengths[me - step], toks, toks, toks
        flat = lengths[jnp.maximum(me - step, 0)]
        joint = cut1 + ends[1]
        at = [step == k for k in range(n)]

        def pick(plain, one, two, three):
            return jnp.where(unpacks, jnp.where(at[1], one, jnp.where(at[2], two, three)), plain)

        return (
            pick(flat, jnp.minimum(ends[2], half), joint - half, jnp.minimum(joint - toks - half, half)),
            pick(toks, half, toks, cut0 - toks - half),
            pick(toks, half + joint, toks, half),
            pick(toks, toks, cut0 - half, jnp.where(short, half + ends[3], toks)),
        )

    def within(at, limits):
        a, b, c, d = limits
        return (at < a) | ((at >= b) & (at < c)) | (at >= d)

    def attend(step, u, shared):
        first = isinstance(step, int)
        g, i = divmod(u, group // part)
        if i == 0:
            lanes_g = slice(g * width, (g + 1) * width)
            lanes_v = slice(kv + g * width, kv + (g + 1) * width)
            if first:
                keys = kvbuf[0, :, lanes_g]
                values = kvbuf[0, :, lanes_v].T
                counted = jnp.ones((pad, toks), bf16)
            else:
                limits = ranges(step)
                key_live = within(tok_col, limits)
                seen = kvbuf[0, 0:1, lanes_g].astype(f32)
                keys = kvbuf[step, :, lanes_g].astype(f32)
                keys = jnp.where(key_live, keys, seen).astype(bf16)
                values = kvbuf[step, :, lanes_v].astype(f32)
                values = jnp.where(key_live, values, 0.0).astype(bf16).T
                counted = jnp.where(within(lane_pos, limits), 1.0, 0.0).astype(bf16)
            shared[:] = [keys, jnp.concatenate([values, counted], axis=0)]
        keys, values = shared
        hs = [g * group + i * part + j for j in range(part)]
        scores = [mm(keys, sq[:, h * width : (h + 1) * width], ((1,), (1,))) for h in hs]
        if first:
            scores = [x + bias[...] for x in scores]
            peaks = [jnp.max(x, axis=0, keepdims=True) for x in scores]
        else:
            olds = [peak[h] for h in hs]
            peaks = [
                jnp.maximum(o, jnp.max(x, axis=0, keepdims=True)) for o, x in zip(olds, scores)
            ]
        probs = [jnp.exp2((x - p) * factor).astype(bf16) for x, p in zip(scores, peaks)]
        sums = [mm(values, x) for x in probs]
        if not first:
            sums = [
                jnp.exp2((o - p) * factor) * acc[h] + x
                for h, o, p, x in zip(hs, olds, peaks, sums)
            ]
        for h, p, x in zip(hs, peaks, sums):
            peak[h] = p
            acc[h] = x

    shared = []
    for u in range(units):
        @pl.when(me > 0)
        def _():
            arrive(1, u)

        attend(0, u, shared)
        hs = range(u * part, (u + 1) * part)
        block_states(hs)
        insides(hs)

        @pl.when(me == 0)
        def _():
            for b in range(u * part // BATCH, (u + 1) * part // BATCH):
                state_copy(b).start()

    if packed:
        state_row = lax.broadcasted_iota(jnp.int32, (width, width), 0)
        result_end = jnp.where(short, ends[3], 0)
        spare_end = jnp.where(short, width, 0)
        across_end = jnp.where(unpacks & short, half, 0)

    relays = (me > 0) & (me < last)
    early = heads // 2

    def later(step, carry):
        if packed:
            @pl.when(unpacks & (step == last))
            def _():
                unpack()

            @pl.when(packs & (step == me))
            def _():
                query_copy.wait_recv()
                moved = mm(one_hot(half, toks, ends[2] - half, toks), kvbuf[0])
                for h in range(tiles):
                    spare[h] = moved[:, h * width : (h + 1) * width]

        shared = []
        for u in range(units):
            @pl.when(step < me)
            def _():
                arrive(step + 1, u)

            @pl.when(relays & (step == me))
            def _():
                each = early // BATCH // units
                for b in range(u * each, (u + 1) * each):
                    pass_states(b)

            attend(step, u, shared)
        return carry

    lax.fori_loop(1, me + 1, later, 0)

    def finish_soft(c, carry):
        hs = [c * FINISH + j for j in range(FINISH)]
        results = [(acc[h, :width, :] / acc[h, width : width + 1, :]).T for h in hs]
        for h, x in zip(hs, results):
            soft_out[:, head_lanes(h)] = jnp.where(live, x, 0.0).astype(bf16)
        return carry

    lax.fori_loop(0, heads // FINISH, finish_soft, 0)

    copies[7].wait()

    @pl.when(me == 0)
    def _():
        state_in[...] = jnp.zeros_like(state_in)

    ends_at = heads - CHUNK
    end_q[...] = lq[:, ends_at * width :]
    for j in range(CHUNK):
        end_sum[j] = insum[ends_at + j]
        end_drop[j] = jnp.exp2(cols[ends_at + j]) * scale
    end_gain[...] = gain[ends_at:, :]
    mask = jnp.where(live, 1.0, 0.0)
    end_mask[...] = jnp.where(tok_col < across_end, mask + 2.0, mask) if packed else mask

    def lightning(c, carry):
        hs = [c * CHUNK + j for j in range(CHUNK)]

        @pl.when(relays & (c < chunks // 2))
        def _():
            for j in range(CHUNK // BATCH):
                pass_states((c * CHUNK + early) // BATCH + j)

        @pl.when((me == last) & (c >= tiles // CHUNK if packed else True))
        def _():
            for j in range(CHUNK // BATCH):
                state_copy(c * (CHUNK // BATCH) + j).wait_recv()

        across = [mm(lq[:, head_lanes(h)], state_in[h]) for h in hs]
        if packed:
            results = [state_in[h].astype(f32) for h in hs]
            results = [jnp.concatenate([x] * (toks // width), axis=0) for x in results]
            across = [jnp.where(tok_col < across_end, x, y) for x, y in zip(results, across)]
        drops = [jnp.exp2(cols[h]) * scale for h in hs]
        combined = [insum[h] + a * d for h, a, d in zip(hs, across, drops)]
        means = [jnp.mean(x * x, axis=1, keepdims=True) for x in combined]
        for h, x, mean in zip(hs, combined, means):
            normed = x * lax.rsqrt(mean + 1e-06) * gain[pl.ds(h, 1), :]
            light_out[:, head_lanes(h)] = jnp.where(live, normed, 0.0).astype(bf16)
        return carry

    lax.fori_loop(0, chunks - 1, lightning, 0)

    @pl.when(me == last)
    def _():
        for j in range(CHUNK // BATCH):
            state_copy(ends_at // BATCH + j).wait_recv()

    for j in range(CHUNK):
        end_state[j] = state_in[ends_at + j]

    if packed:
        @pl.when(unpacks)
        def _():
            query_copy.wait_send()

        @pl.when(packs)
        def _():
            front_copy.wait_send()

    @pl.when(me < n - 1)
    def _():
        def sent_blocks(step, carry):
            for p in range(PIECES):
                low = p < PIECES // 2
                front = (step < n - 2) & ((step > 0) | (not low)) | (step == n - 2) & low
                sent = True if not packed else (me < n - 2) | front

                @pl.when(sent)
                def _():
                    kv_copy(step, p).wait_send()

            return carry

        lax.fori_loop(0, me + 1, sent_blocks, 0)

        def sent_states(b, carry):
            state_copy(b).wait_send()
            return carry

        lax.fori_loop(0, heads // BATCH, sent_states, 0)


def finish(
    light, soft, end_q, end_state, end_sum, end_drop, end_mask, end_gain,
    light_hbm, soft_hbm, ready, sem,
):
    toks, width = end_mask.shape
    done = light.shape[1] - end_q.shape[1]
    f32 = jnp.float32
    copies = [
        pltpu.make_async_copy(soft, soft_hbm, sem.at[0]),
        pltpu.make_async_copy(light.at[:, :done], light_hbm.at[:, :done], sem.at[1]),
        pltpu.make_async_copy(ready, light_hbm.at[:, done:], sem.at[2]),
    ]
    copies[0].start()
    copies[1].start()
    mask = end_mask[...]
    spans = [slice(j * width, (j + 1) * width) for j in range(CHUNK)]
    across = [mm(end_q[:, span], end_state[j]) for j, span in enumerate(spans)]
    given = [end_state[j].astype(f32) for j in range(CHUNK)]
    given = [jnp.concatenate([x] * (toks // width), axis=0) for x in given]
    across = [jnp.where(mask > 1.5, x, y) for x, y in zip(given, across)]
    combined = [end_sum[j] + x * end_drop[j] for j, x in enumerate(across)]
    means = [jnp.mean(x * x, axis=1, keepdims=True) for x in combined]
    live = (mask == 1.0) | (mask == 3.0)
    for j, (x, mean) in enumerate(zip(combined, means)):
        normed = x * lax.rsqrt(mean + 1e-06) * end_gain[j : j + 1, :]
        ready[:, spans[j]] = jnp.where(live, normed, 0.0).astype(jnp.bfloat16)
    copies[2].start()
    for copy in copies:
        copy.wait()


def body(n, lq, lk, lv, decay, gain, sq, sk, sv, lengths):
    toks, heads = decay.shape
    width = lq.shape[1] // heads
    kv = sk.shape[1]
    chunks = heads // CHUNK
    bf16, f32 = jnp.bfloat16, jnp.float32
    out = pltpu.VMEM(lq.shape, bf16)
    dma = pltpu.SemaphoreType.DMA
    anywhere = pl.BlockSpec(memory_space=pltpu.HBM)
    vmem = pl.BlockSpec(memory_space=pltpu.VMEM)
    ends = CHUNK * width
    left = pl.pallas_call(
        functools.partial(kernel, n, width),
        out_shape=(
            out, out, pltpu.VMEM((toks, ends), bf16), pltpu.VMEM((CHUNK, width, width), bf16),
            pltpu.VMEM((CHUNK, toks, width), f32), pltpu.VMEM((CHUNK, toks, width), f32),
            pltpu.VMEM((toks, width), f32), pltpu.VMEM((CHUNK, width), f32),
        ),
        in_specs=[anywhere] * 9,
        out_specs=(vmem,) * 8,
        scratch_shapes=[
            pltpu.SMEM(lengths.shape, lengths.dtype),
            pltpu.VMEM(lq.shape, bf16), pltpu.VMEM(lq.shape, bf16), pltpu.VMEM(lq.shape, bf16),
            pltpu.VMEM(sq.shape, bf16), pltpu.VMEM((heads, toks), f32),
            pltpu.VMEM((heads, width), f32),
            pltpu.VMEM((n, toks, 2 * kv), bf16),
            pltpu.VMEM((width, toks), f32), pltpu.VMEM((heads, toks, width), f32),
            pltpu.VMEM((heads, toks), f32),
            pltpu.VMEM((heads, width, width), f32),
            pltpu.VMEM((heads, width, width), bf16), pltpu.VMEM((heads, width, width), bf16),
            pltpu.VMEM((toks, toks), f32), pltpu.VMEM((toks, toks), f32),
            pltpu.VMEM((heads, toks, width), f32),
            pltpu.VMEM((heads, width + 16, toks), f32), pltpu.VMEM((heads, 1, toks), f32),
            pltpu.VMEM((2 * toks, 2 * kv), bf16), pltpu.VMEM((2 * kv // width, toks // 2, width), f32),
            pltpu.VMEM((toks // 2, lq.shape[1]), bf16),
            dma((9,)), dma((n, PIECES)), dma((n, PIECES)), dma((heads // BATCH,)), dma((heads // BATCH,)), dma, dma,
        ],
        compiler_params=pltpu.CompilerParams(
            collective_id=0, has_side_effects=True, vmem_limit_bytes=58000000
        ),
        name="hybrid",
    )(lq, lk, lv, decay.T, gain.reshape(heads, width), sq, sk, sv, lengths)
    whole = jax.ShapeDtypeStruct(lq.shape, bf16)
    return pl.pallas_call(
        finish,
        out_shape=(whole, whole),
        in_specs=[vmem] * 8,
        out_specs=(anywhere, anywhere),
        scratch_shapes=[pltpu.VMEM((toks, ends), bf16), dma((3,))],
        compiler_params=pltpu.CompilerParams(vmem_limit_bytes=4000000),
        name="finish",
    )(*left)


def solution(mesh):
    block = P(("groups", "seq"), ("section", "mp"))
    return jax.shard_map(
        functools.partial(body, mesh.shape["seq"]),
        mesh=mesh,
        in_specs=(block, block, block, block, P(("section", "mp")), block, block, block, P("groups")),
        out_specs=(block, block),
        check_vma=False,
    )
```
